32 devices in a mesh: seq: 4 (over y, x), tp: 8 (over z, core).
Axes of the slice: x: 2, y: 2, z: 4, core: 2. Of those that a mesh axis runs over, the one named last changes fastest.
Arguments:
- tokens: bfloat16 [1024, 4096], P('seq', 'tp'), may hold values from -30 to 30
- w_qkv: bfloat16 [4096, 3, 2048], P('seq', None, 'tp'), may hold values from -1 to 1
- keep_list: int32 [512], P('seq'), may hold values from 0 to 255, as said below
- counts: int32 [4], P('seq'), may hold values from 1 to 127, as said below
Outputs:
- attended: bfloat16 [256, 2048], P('seq', 'tp')
The draws below stay inside these ranges and needn't reach their ends.
Inputs may be any that keep to these rules, and one draw needn't show every extreme that they name: `counts`: the entries sum to 256; one shard keeps 2 * 64 - 1 tokens and one shard keeps 1. `keep_list`: entries s * 2 * 64 to s * 2 * 64 + 2 * 64 - 1 are distinct token indices within shard s; the first counts[s] of them increase.
All inputs are finite; a program needn't handle non-finite values.
Results may differ from the reference program's by a relative error of at most 0.0065.
Values may be sent and summed in bfloat16 or wider, within the bound.
No kernel may reach another device: no remote copies, remote signals or barrier semaphores. Data moves between devices by JAX's collectives and lax.ppermute only.
A program may use at most 64 MiB of HBM per device.

```python
import jax
import jax.numpy as jnp
from jax import lax

D = 4096
HEADS = 16
HD = 128
TOK_DEV = 256
CAP = 64
TOKENS = 1024
KEPT = 256


def keep_plan(key):
    shards = KEPT // CAP
    base = jax.random.fold_in(key, 11)
    pick_key, shift_key, perm_key = jax.random.split(base, 3)
    order = jax.random.permutation(pick_key, shards)
    shift = jax.random.randint(shift_key, (shards // 2,), 0, CAP).astype(jnp.int32)
    shift = shift.at[0].set(CAP - 1)
    counts = jnp.zeros((shards,), jnp.int32)
    counts = counts.at[order[:shards // 2]].set(CAP + shift)
    counts = counts.at[order[shards // 2:]].set(CAP - shift)
    row_keys = jax.random.split(perm_key, shards)
    chosen = jax.vmap(lambda single: jax.random.permutation(single, TOK_DEV)[:2 * CAP])(row_keys)
    slot_ids = jnp.arange(2 * CAP, dtype=jnp.int32)
    ranked = jnp.where(slot_ids[None, :] < counts[:, None], chosen, chosen + TOK_DEV)
    keep = jnp.sort(ranked, axis=1) % TOK_DEV
    return (counts, keep.reshape(-1).astype(jnp.int32))


def draw_counts(key, part):
    return keep_plan(key)[0]


def draw_keep_list(key, part):
    return keep_plan(key)[1]


def draw_tokens(key, part):
    first_key = jax.random.fold_in(key, 0)
    values = jax.random.normal(first_key, (TOKENS, D), jnp.float32)
    return jnp.clip(values, -6.0, 6.0).astype(jnp.bfloat16)


def draw_w_qkv(key, part):
    values = jax.random.normal(key, (D, 3, HEADS * HD), jnp.float32) * D ** (-0.5)
    return jnp.clip(values, -1.0, 1.0).astype(jnp.bfloat16)


def setup_inputs(seed: int = 0) -> dict:
    seeds = jax.random.split(jax.random.key(seed), 5)
    return {
        "tokens": draw_tokens(jax.random.fold_in(seeds[4], 71), 0),
        "w_qkv": draw_w_qkv(jax.random.fold_in(seeds[4], 71), 0),
        "keep_list": draw_keep_list(jax.random.fold_in(seeds[4], 71), 0),
        "counts": draw_counts(jax.random.fold_in(seeds[4], 71), 0),
    }


def reference(tokens, w_qkv, keep_list, counts):
    shards = counts.shape[0]
    tok_dev = tokens.shape[0] // shards
    slots = keep_list.shape[0] // shards
    kept_total = shards * CAP
    ends = jnp.cumsum(counts).astype(jnp.int32)
    starts = (ends - counts).astype(jnp.int32)
    rows = jnp.arange(kept_total, dtype=jnp.int32)
    ranks = (rows % CAP) * shards + rows // CAP
    source = jnp.sum((ends[None, :] <= ranks[:, None]).astype(jnp.int32), axis=1).astype(jnp.int32)
    within = ranks - starts[source]
    local = keep_list[source * slots + within]
    positions = (source * tok_dev + local).astype(jnp.int32)
    chosen = tokens[positions]
    projected = jnp.dot(chosen, w_qkv.reshape(D, 3 * HEADS * HD), preferred_element_type=jnp.float32)
    projected = projected.astype(jnp.bfloat16).reshape(kept_total, 3, HEADS, HD)
    heads_first = jnp.transpose(projected, (2, 1, 0, 3))
    causal = positions[None, :] > positions[:, None]

    def one_head(block):
        scores = jnp.dot(block[0], block[1].T, preferred_element_type=jnp.float32) * (HD ** -0.5)
        scores = jnp.where(causal, -jnp.inf, scores)
        top = jnp.max(scores, axis=1, keepdims=True)
        expo = jnp.exp(scores - top)
        weights = expo.astype(jnp.bfloat16)
        numer = jnp.dot(weights, block[2], preferred_element_type=jnp.float32)
        return numer / jnp.sum(expo, axis=1)[:, None]

    outputs = lax.map(one_head, heads_first)
    return jnp.transpose(outputs, (1, 0, 2)).reshape(kept_total, HEADS * HD).astype(jnp.bfloat16)
```

```python
import functools

import jax
import jax.numpy as jnp
from jax import lax
from jax.experimental import pallas as pl
from jax.experimental.pallas import tpu as pltpu
from jax.sharding import PartitionSpec as P

HD = 128


def entering(value, axis, join, neutral):
    count, mine = (lax.axis_size(axis), lax.axis_index(axis))
    pieces = lax.all_gather(value, axis)
    so_far = jnp.full_like(value, 0) + jnp.asarray(neutral, value.dtype)

    def lap(position, so_far):
        longer = join(so_far, pieces[position])
        return jnp.where(position < mine, longer, so_far)

    return lax.fori_loop(0, count - 1, lap, so_far)


def add_sums(earlier, later):
    return earlier + later


def by_rows(tokens, w_qkv, keep_list, counts):
    shards = lax.axis_size("seq")
    my_index = lax.axis_index("seq")
    tok_dev = tokens.shape[0]
    slots = keep_list.shape[0]
    capacity = slots // 2
    per_peer = slots // shards
    head_dim = HD
    columns = w_qkv.shape[2]
    local_heads = columns // head_dim
    offset = entering(counts, "seq", add_sums, jnp.zeros_like(counts))[0]
    peers = jnp.arange(shards, dtype=jnp.int32)[:, None]
    rounds = jnp.arange(per_peer, dtype=jnp.int32)[None, :]
    local_slot = (peers - offset) % shards + rounds * shards
    live = local_slot < counts[0]
    token_index = keep_list[local_slot]
    ranks = jnp.where(live, offset + local_slot, -1).astype(jnp.int32)
    positions = my_index * tok_dev + token_index
    meta = jnp.stack([positions, ranks], axis=2)
    picked = jnp.where(live[:, :, None], tokens[token_index], jnp.zeros((), tokens.dtype))
    arrived, arrived_meta = (
        lax.all_to_all(picked, "seq", split_axis=0, concat_axis=0, tiled=True),
        lax.all_to_all(meta, "seq", split_axis=0, concat_axis=0, tiled=True),
    )
    arrived_meta = arrived_meta.reshape(shards * per_peer, 2)
    arrived_rank = arrived_meta[:, 1]
    target = jnp.where(arrived_rank >= 0, arrived_rank // shards, capacity)
    flat = arrived.reshape(shards * per_peer, arrived.shape[2])
    kept = jnp.zeros((capacity, flat.shape[1]), flat.dtype).at[target].set(flat, mode="drop")
    kept_pos = jnp.zeros((capacity,), jnp.int32).at[target].set(arrived_meta[:, 0], mode="drop")
    full_rows = lax.all_gather(kept, "tp", axis=1, tiled=True)
    piece = lax.all_gather(w_qkv, "seq", axis=0, tiled=True)
    part_rows = lax.slice_in_dim(full_rows, 0, piece.shape[0], axis=1)
    projected = jnp.einsum(
        "rd,dgc->rgc", part_rows, piece, preferred_element_type=jnp.float32
    ).astype(jnp.bfloat16)
    queries = projected[:, 0].reshape(capacity, local_heads, head_dim)
    key_values = projected[:, 1:]
    scale = head_dim ** (-0.5)
    all_kv, all_pos = (
        lax.all_gather(key_values, "seq", axis=0, tiled=True),
        lax.all_gather(kept_pos, "seq", axis=0, tiled=True),
    )
    total_keys = all_kv.shape[0]
    keys_all = all_kv[:, 0].reshape(total_keys, local_heads, head_dim)
    values_all = all_kv[:, 1].reshape(total_keys, local_heads, head_dim)
    scores = (
        jnp.einsum("qhd,khd->hqk", queries, keys_all, preferred_element_type=jnp.float32) * scale
    )
    masked = all_pos[None, None, :] > kept_pos[None, :, None]
    scores = jnp.where(masked, -jnp.inf, scores)
    top = jnp.max(scores, axis=2, keepdims=True)
    expo = jnp.exp(scores - top)
    numer = jnp.einsum(
        "hqk,khd->hqd", expo.astype(jnp.bfloat16), values_all, preferred_element_type=jnp.float32
    )
    result = numer / jnp.sum(expo, axis=2)[..., None]
    return jnp.transpose(result, (1, 0, 2)).reshape(capacity, columns).astype(jnp.bfloat16)


VMEM = pl.BlockSpec(memory_space=pltpu.VMEM)
SMEM = pl.BlockSpec(memory_space=pltpu.SMEM)


def gather_kernel(counts_ref, keep_ref, tokens_ref, out_ref):
    slots = out_ref.shape[0]
    tok_dev = tokens_ref.shape[0]
    token = lax.broadcasted_iota(jnp.int32, (tok_dev, slots), 0)
    pick = (token == keep_ref[...]).astype(jnp.bfloat16)
    rows = lax.dot_general(
        pick, tokens_ref[...], (((0,), (0,)), ((), ())), preferred_element_type=jnp.float32
    )
    count = counts_ref[0].astype(jnp.float32)
    last = lax.broadcasted_iota(jnp.int32, rows.shape, 0) == slots - 1
    out_ref[...] = jnp.where(last, count, rows).astype(jnp.bfloat16)


def project_kernel(shards, group, heads, *refs):
    total = shards
    halves = [refs[total * p : total * (p + 1)] for p in range(group)]
    w_ref = refs[total * group]
    outs = refs[total * group + 1 :]
    slots, width = halves[0][0].shape
    capacity = slots // 2
    kept = capacity * shards
    tp = lax.axis_index("tp")
    core = lax.rem(tp, group)
    line = lax.div(tp, group)
    me = lax.axis_index("seq")
    shard = [lax.rem(line - k + shards, shards) for k in range(total)]
    count = [halves[0][k][slots - 1 : slots, :slots].astype(jnp.float32) for k in range(total)]
    row = lax.broadcasted_iota(jnp.int32, (kept, slots), 0)
    rank = ((row % capacity) * shards + row // capacity).astype(jnp.float32)
    slot = lax.broadcasted_iota(jnp.int32, (kept, slots), 1).astype(jnp.float32)
    picks = []
    for k in range(total):
        start = jnp.zeros_like(count[k])
        for j in range(total):
            if j != k:
                start += jnp.where(shard[j] < shard[k], count[j], 0.0)
        hit = (rank == slot + start) & (slot < count[k])
        picks.append(jnp.where(hit, 1.0, 0.0).astype(jnp.bfloat16))
    rows = []
    for p in range(group):
        total_rows = None
        for k in range(total):
            part = jnp.dot(picks[k], halves[p][k][...], preferred_element_type=jnp.float32)
            total_rows = part if total_rows is None else total_rows + part
        rows.append(total_rows.astype(jnp.bfloat16))

    def times(kind, head, which):
        acc = None
        for p in range(group):
            where = pl.multiple_of(lax.rem(core + p, group) * width, width)
            w = w_ref[kind, pl.ds(where, width), head * HD : (head + 1) * HD]
            part = jnp.dot(which[p], w, preferred_element_type=jnp.float32)
            acc = part if acc is None else acc + part
        return acc.astype(jnp.bfloat16)

    blocks = shards // heads
    block_rows = kept // blocks
    for head in range(heads):
        key = times(1, head, rows)
        value = times(2, head, rows)
        query = times(0, head, rows)
        for k in range(shards):
            dest = lax.rem(me + k, shards)
            block = lax.div(dest, heads)

            @pl.when(lax.rem(dest, heads) == head)
            def _(k=k, block=block):
                outs[k][0:kept, :] = key
                outs[k][kept : 2 * kept, :] = value
                for b in range(blocks):

                    @pl.when(block == b)
                    def _(b=b):
                        outs[k][2 * kept :, :] = query[b * block_rows : (b + 1) * block_rows, :]


def attend_kernel(shards, heads, kept, *refs):
    parts, outs = refs[:shards], refs[shards:]
    capacity = kept // shards
    me = lax.axis_index("seq")
    block_rows = parts[0].shape[0] - 2 * kept
    block = lax.div(me, heads)

    def summed(lo, hi):
        acc = parts[0][lo:hi, :].astype(jnp.float32)
        for p in parts[1:]:
            acc += p[lo:hi, :].astype(jnp.float32)
        return acc.astype(jnp.bfloat16)

    key, value, query = summed(0, kept), summed(kept, 2 * kept), summed(2 * kept, 2 * kept + block_rows)
    scores = lax.dot_general(
        query, key, (((1,), (1,)), ((), ())), preferred_element_type=jnp.float32
    ) * (HD ** (-0.5))
    q_row = lax.broadcasted_iota(jnp.int32, scores.shape, 0) + block * block_rows
    k_row = lax.broadcasted_iota(jnp.int32, scores.shape, 1)
    q_rank = lax.rem(q_row, capacity) * shards + lax.div(q_row, capacity)
    k_rank = lax.rem(k_row, capacity) * shards + lax.div(k_row, capacity)
    scores = jnp.where(k_rank > q_rank, -jnp.inf, scores)
    top = jnp.max(scores, axis=1, keepdims=True)
    expo = jnp.exp(scores - top)
    numer = jnp.dot(expo.astype(jnp.bfloat16), value, preferred_element_type=jnp.float32)
    result = (numer / jnp.sum(expo, axis=1, keepdims=True)).astype(jnp.bfloat16)
    head = lax.rem(me, heads)
    for k in range(heads):
        owner = lax.rem(head + k, heads)
        for o in range(heads):

            @pl.when(owner == o)
            def _(k=k, o=o):
                outs[k][...] = result[o * capacity : (o + 1) * capacity, :]


def by_features(shards, tp, tokens, w_qkv, keep_list, counts):
    group = tp // shards
    slots = keep_list.shape[0]
    capacity = slots // 2
    kept = capacity * shards
    width = tokens.shape[1]
    heads = w_qkv.shape[2] // HD
    blocks = shards // heads
    params = pltpu.CompilerParams(vmem_limit_bytes=32 * 1024 * 1024)
    packed = pl.pallas_call(
        gather_kernel,
        out_shape=jax.ShapeDtypeStruct((slots, width), jnp.bfloat16),
        in_specs=[SMEM, VMEM, VMEM],
        out_specs=VMEM,
        compiler_params=params,
        name="gather",
    )(counts, keep_list.reshape(1, slots), tokens)

    def device(s, line, core):
        return s * tp + line * group + core

    every = [(s, line, c) for s in range(shards) for line in range(shards) for c in range(group)]
    own = [
        lax.ppermute(
            packed,
            ("seq", "tp"),
            [(device(s, line, c), device(line, (s + k) % shards, c)) for s, line, c in every],
        )
        for k in range(shards)
    ]
    halves = list(own)
    for p in range(1, group):
        halves += [
            lax.ppermute(
                chunk,
                "tp",
                [
                    (line * group + (c + p) % group, line * group + c)
                    for line in range(shards)
                    for c in range(group)
                ],
            )
            for chunk in own
        ]
    payload = 2 * kept + kept // blocks
    partial = pl.pallas_call(
        functools.partial(project_kernel, shards, group, heads),
        out_shape=[jax.ShapeDtypeStruct((payload, HD), jnp.bfloat16)] * shards,
        in_specs=[VMEM] * (shards * group + 1),
        out_specs=[VMEM] * shards,
        compiler_params=params,
        name="project",
    )(*halves, jnp.transpose(w_qkv, (1, 0, 2)))
    parts = [partial[0]] + [
        lax.ppermute(partial[k], "seq", [(s, (s + k) % shards) for s in range(shards)])
        for k in range(1, shards)
    ]
    pieces = pl.pallas_call(
        functools.partial(attend_kernel, shards, heads, kept),
        out_shape=[jax.ShapeDtypeStruct((capacity, HD), jnp.bfloat16)] * heads,
        in_specs=[VMEM] * shards,
        out_specs=[VMEM] * heads,
        compiler_params=params,
        name="attend",
    )(*parts)
    arrived = [pieces[0]] + [
        lax.ppermute(
            pieces[k],
            "seq",
            [(b * heads + h, b * heads + (h + k) % heads) for b in range(blocks) for h in range(heads)],
        )
        for k in range(1, heads)
    ]
    mine = lax.rem(lax.axis_index("seq"), heads)
    columns = []
    for h in range(heads):
        column = arrived[0]
        for k in range(1, heads):
            column = jnp.where(lax.rem(mine - k + heads, heads) == h, arrived[k], column)
        columns.append(column)
    return jnp.concatenate(columns, axis=1)


def solution(mesh):
    shards, tp = mesh.shape["seq"], mesh.shape["tp"]

    def on_device(tokens, w_qkv, keep_list, counts):
        heads = w_qkv.shape[2] // HD
        if tp % shards == 0 and shards % heads == 0:
            return by_features(shards, tp, tokens, w_qkv, keep_list, counts)
        return by_rows(tokens, w_qkv, keep_list, counts)

    in_specs = (P("seq", "tp"), P("seq", None, "tp"), P("seq"), P("seq"))
    out_specs = P("seq", "tp")
    return jax.shard_map(
        on_device, mesh=mesh, in_specs=in_specs, out_specs=out_specs, check_vma=False
    )
```

```python
import functools

import jax
import jax.numpy as jnp
from jax import lax
from jax.experimental import pallas as pl
from jax.experimental.pallas import tpu as pltpu
from jax.sharding import PartitionSpec as P

HD = 128


def entering(value, axis, join, neutral):
    count, mine = (lax.axis_size(axis), lax.axis_index(axis))
    pieces = lax.all_gather(value, axis)
    so_far = jnp.full_like(value, 0) + jnp.asarray(neutral, value.dtype)

    def lap(position, so_far):
        longer = join(so_far, pieces[position])
        return jnp.where(position < mine, longer, so_far)

    return lax.fori_loop(0, count - 1, lap, so_far)


def add_sums(earlier, later):
    return earlier + later


def by_rows(tokens, w_qkv, keep_list, counts):
    shards = lax.axis_size("seq")
    my_index = lax.axis_index("seq")
    tok_dev = tokens.shape[0]
    slots = keep_list.shape[0]
    capacity = slots // 2
    per_peer = slots // shards
    head_dim = HD
    columns = w_qkv.shape[2]
    local_heads = columns // head_dim
    offset = entering(counts, "seq", add_sums, jnp.zeros_like(counts))[0]
    peers = jnp.arange(shards, dtype=jnp.int32)[:, None]
    rounds = jnp.arange(per_peer, dtype=jnp.int32)[None, :]
    local_slot = (peers - offset) % shards + rounds * shards
    live = local_slot < counts[0]
    token_index = keep_list[local_slot]
    ranks = jnp.where(live, offset + local_slot, -1).astype(jnp.int32)
    positions = my_index * tok_dev + token_index
    meta = jnp.stack([positions, ranks], axis=2)
    picked = jnp.where(live[:, :, None], tokens[token_index], jnp.zeros((), tokens.dtype))
    arrived, arrived_meta = (
        lax.all_to_all(picked, "seq", split_axis=0, concat_axis=0, tiled=True),
        lax.all_to_all(meta, "seq", split_axis=0, concat_axis=0, tiled=True),
    )
    arrived_meta = arrived_meta.reshape(shards * per_peer, 2)
    arrived_rank = arrived_meta[:, 1]
    target = jnp.where(arrived_rank >= 0, arrived_rank // shards, capacity)
    flat = arrived.reshape(shards * per_peer, arrived.shape[2])
    kept = jnp.zeros((capacity, flat.shape[1]), flat.dtype).at[target].set(flat, mode="drop")
    kept_pos = jnp.zeros((capacity,), jnp.int32).at[target].set(arrived_meta[:, 0], mode="drop")
    full_rows = lax.all_gather(kept, "tp", axis=1, tiled=True)
    piece = lax.all_gather(w_qkv, "seq", axis=0, tiled=True)
    part_rows = lax.slice_in_dim(full_rows, 0, piece.shape[0], axis=1)
    projected = jnp.einsum(
        "rd,dgc->rgc", part_rows, piece, preferred_element_type=jnp.float32
    ).astype(jnp.bfloat16)
    queries = projected[:, 0].reshape(capacity, local_heads, head_dim)
    key_values = projected[:, 1:]
    scale = head_dim ** (-0.5)
    all_kv, all_pos = (
        lax.all_gather(key_values, "seq", axis=0, tiled=True),
        lax.all_gather(kept_pos, "seq", axis=0, tiled=True),
    )
    total_keys = all_kv.shape[0]
    keys_all = all_kv[:, 0].reshape(total_keys, local_heads, head_dim)
    values_all = all_kv[:, 1].reshape(total_keys, local_heads, head_dim)
    scores = (
        jnp.einsum("qhd,khd->hqk", queries, keys_all, preferred_element_type=jnp.float32) * scale
    )
    masked = all_pos[None, None, :] > kept_pos[None, :, None]
    scores = jnp.where(masked, -jnp.inf, scores)
    top = jnp.max(scores, axis=2, keepdims=True)
    expo = jnp.exp(scores - top)
    numer = jnp.einsum(
        "hqk,khd->hqd", expo.astype(jnp.bfloat16), values_all, preferred_element_type=jnp.float32
    )
    result = numer / jnp.sum(expo, axis=2)[..., None]
    return jnp.transpose(result, (1, 0, 2)).reshape(capacity, columns).astype(jnp.bfloat16)


VMEM = pl.BlockSpec(memory_space=pltpu.VMEM)
HBM = pl.BlockSpec(memory_space=pltpu.HBM)
TOP_BITS = 14


def gather(tokens, keep_list, counts):
    slots = keep_list.shape[0]
    token = lax.broadcasted_iota(jnp.int32, (tokens.shape[0], slots), 0)
    pick = (token == keep_list[None, :]).astype(jnp.bfloat16)
    rows = lax.dot_general(pick, tokens, (((0,), (0,)), ((), ())), preferred_element_type=jnp.float32)
    last = lax.broadcasted_iota(jnp.int32, rows.shape, 0) == slots - 1
    return jnp.where(last, counts[0].astype(jnp.float32), rows).astype(jnp.bfloat16)


def load_kernel(after_hbm, w_hbm, out_ref, sem):
    del after_hbm
    copy = pltpu.make_async_copy(w_hbm, out_ref, sem)
    copy.start()
    copy.wait()


def project_kernel(shards, group, heads, *refs):
    halves = [refs[shards * p : shards * (p + 1)] for p in range(group)]
    w_ref = refs[shards * group]
    outs = refs[shards * group + 1 :]
    slots, width = halves[0][0].shape
    capacity = slots // 2
    kept = capacity * shards
    stride = core_stride(shards, group)
    tp = lax.axis_index("tp")
    core = lax.rem(tp, group)
    line = lax.div(tp, group)
    me = lax.axis_index("seq")
    shard = [lax.rem(line - k - core * stride + 2 * shards, shards) for k in range(shards)]
    count = [halves[0][k][slots - 1 : slots, :slots].astype(jnp.float32) for k in range(shards)]
    row = lax.broadcasted_iota(jnp.int32, (kept, slots), 0)
    rank = ((row % capacity) * shards + row // capacity).astype(jnp.float32)
    slot = lax.broadcasted_iota(jnp.int32, (kept, slots), 1).astype(jnp.float32)
    first = rank - slot
    picks = []
    for k in range(shards):
        start = jnp.zeros_like(count[k])
        for j in range(shards):
            if j != k:
                start += jnp.where(shard[j] < shard[k], count[j], 0.0)
        hit = (first == start) & (slot < count[k])
        picks.append(jnp.where(hit, 1.0, 0.0).astype(jnp.bfloat16))
    rows = []
    for p in range(group):
        pick = jnp.concatenate([picks[(k + p * stride) % shards] for k in range(shards)], axis=1)
        block = jnp.concatenate([halves[p][k][...] for k in range(shards)], axis=0)
        rows.append(jnp.dot(pick, block, preferred_element_type=jnp.float32).astype(jnp.bfloat16))
    blocks = shards // heads
    block_rows = kept // blocks
    total = 2 * kept + block_rows
    pad = outs[0].shape[0] - total
    exponents = []
    for kind, lo in ((1, 0), (2, kept), (0, 2 * kept)):
        acc = None
        for p in range(group):
            where = pl.multiple_of(lax.rem(core + p, group) * width, width)
            part = jnp.dot(
                rows[p], w_ref[kind, pl.ds(where, width), :], preferred_element_type=jnp.float32
            )
            acc = part if acc is None else acc + part
        most = jnp.maximum(jnp.max(jnp.abs(acc), axis=0, keepdims=True), 2.0**-100)
        exponent = jnp.floor(jnp.log2(most)) + 1.0
        exponents.append(exponent)
        value = jnp.round(acc * jnp.exp2(TOP_BITS - exponent)).astype(jnp.int32).astype(jnp.int16)
        for k in range(shards):
            dest = lax.rem(me + k, shards)
            for head in range(heads):
                mine = value[:, head * HD : (head + 1) * HD]
                if kind:

                    @pl.when(lax.rem(dest, heads) == head)
                    def _(k=k, lo=lo, mine=mine):
                        outs[k][lo : lo + kept, :] = mine
                else:
                    for b in range(blocks):

                        @pl.when(dest == b * heads + head)
                        def _(k=k, lo=lo, b=b, mine=mine):
                            outs[k][lo:total, :] = mine[b * block_rows : (b + 1) * block_rows, :]

    index = lax.broadcasted_iota(jnp.int32, (pad, HD), 0)
    for k in range(shards):
        dest = lax.rem(me + k, shards)
        for head in range(heads):

            @pl.when(lax.rem(dest, heads) == head)
            def _(k=k, head=head):
                tail = jnp.zeros((pad, HD), jnp.float32)
                for i, exponent in enumerate(exponents):
                    tail = jnp.where(index == i, exponent[:, head * HD : (head + 1) * HD], tail)
                outs[k][total:, :] = tail.astype(jnp.int32).astype(jnp.int16)


def attend_kernel(shards, heads, kept, *refs):
    parts, outs = refs[:shards], refs[shards:]
    capacity = kept // shards
    me = lax.axis_index("seq")
    block_rows = kept // (shards // heads)
    total = 2 * kept + block_rows
    block = lax.div(me, heads)
    scales = [
        jnp.exp2(p[total:, :].astype(jnp.int32).astype(jnp.float32) - TOP_BITS) for p in parts
    ]

    def summed(i, lo, hi):
        acc = None
        for p, scale in zip(parts, scales):
            part = p[lo:hi, :].astype(jnp.int32).astype(jnp.float32) * scale[i : i + 1, :]
            acc = part if acc is None else acc + part
        return acc.astype(jnp.bfloat16)

    key, value, query = summed(0, 0, kept), summed(1, kept, 2 * kept), summed(2, 2 * kept, total)
    scores = lax.dot_general(
        query, key, (((1,), (1,)), ((), ())), preferred_element_type=jnp.float32
    ) * (HD ** (-0.5))
    q_row = lax.broadcasted_iota(jnp.int32, scores.shape, 0) + block * block_rows
    k_row = lax.broadcasted_iota(jnp.int32, scores.shape, 1)
    q_rank = lax.rem(q_row, capacity) * shards + lax.div(q_row, capacity)
    k_rank = lax.rem(k_row, capacity) * shards + lax.div(k_row, capacity)
    scores = jnp.where(k_rank > q_rank, -jnp.inf, scores)
    top = jnp.max(scores, axis=1, keepdims=True)
    expo = jnp.exp(scores - top)
    numer = jnp.dot(expo.astype(jnp.bfloat16), value, preferred_element_type=jnp.float32)
    result = (numer / jnp.sum(expo, axis=1, keepdims=True)).astype(jnp.bfloat16)
    head = lax.rem(me, heads)
    for k in range(heads):
        owner = lax.rem(head + k, heads)
        for o in range(heads):

            @pl.when(owner == o)
            def _(k=k, o=o):
                outs[k][...] = result[o * capacity : (o + 1) * capacity, :]


def core_stride(shards, group):
    return shards // group if shards % group == 0 else 0


def by_features(shards, tp, tokens, w_qkv, keep_list, counts):
    group = tp // shards
    slots = keep_list.shape[0]
    capacity = slots // 2
    kept = capacity * shards
    heads = w_qkv.shape[2] // HD
    blocks = shards // heads
    params = pltpu.CompilerParams(vmem_limit_bytes=32 * 1024 * 1024)
    packed = gather(tokens, keep_list, counts)

    def device(s, line, core):
        return s * tp + line * group + core

    stride = core_stride(shards, group)
    every = [(s, line, c) for s in range(shards) for line in range(shards) for c in range(group)]
    own = [
        lax.ppermute(
            packed,
            ("seq", "tp"),
            [
                (device(s, line, c), device(line, (s + k + c * stride) % shards, c))
                for s, line, c in every
            ],
        )
        for k in range(shards)
    ]
    halves = list(own)
    for p in range(1, group):
        halves += [
            lax.ppermute(
                chunk,
                "tp",
                [
                    (line * group + (c + p) % group, line * group + c)
                    for line in range(shards)
                    for c in range(group)
                ],
            )
            for chunk in own
        ]
    weights = jnp.transpose(w_qkv, (1, 0, 2))
    weights = pl.pallas_call(
        load_kernel,
        out_shape=jax.ShapeDtypeStruct(weights.shape, weights.dtype),
        in_specs=[pl.BlockSpec(memory_space=pl.ANY), HBM],
        out_specs=VMEM,
        scratch_shapes=[pltpu.SemaphoreType.DMA],
        compiler_params=pltpu.CompilerParams(vmem_limit_bytes=51 * 1024 * 1024),
        name="load",
    )(own[0], weights)
    payload = 2 * kept + kept // blocks + 16
    partial = pl.pallas_call(
        functools.partial(project_kernel, shards, group, heads),
        out_shape=[jax.ShapeDtypeStruct((payload, HD), jnp.int16)] * shards,
        in_specs=[VMEM] * (shards * group + 1),
        out_specs=[VMEM] * shards,
        compiler_params=params,
        name="project",
    )(*halves, weights)
    parts = [partial[0]] + [
        lax.ppermute(partial[k], "seq", [(s, (s + k) % shards) for s in range(shards)])
        for k in range(1, shards)
    ]
    pieces = pl.pallas_call(
        functools.partial(attend_kernel, shards, heads, kept),
        out_shape=[jax.ShapeDtypeStruct((capacity, HD), jnp.bfloat16)] * heads,
        in_specs=[VMEM] * shards,
        out_specs=[VMEM] * heads,
        compiler_params=params,
        name="attend",
    )(*parts)
    arrived = [pieces[0]] + [
        lax.ppermute(
            pieces[k],
            "seq",
            [(b * heads + h, b * heads + (h + k) % heads) for b in range(blocks) for h in range(heads)],
        )
        for k in range(1, heads)
    ]
    mine = lax.rem(lax.axis_index("seq"), heads)
    columns = []
    for h in range(heads):
        column = arrived[0]
        for k in range(1, heads):
            column = jnp.where(lax.rem(mine - k + heads, heads) == h, arrived[k], column)
        columns.append(column)
    return jnp.concatenate(columns, axis=1)


def solution(mesh):
    shards, tp = mesh.shape["seq"], mesh.shape["tp"]

    def on_device(tokens, w_qkv, keep_list, counts):
        heads = w_qkv.shape[2] // HD
        if tp % shards == 0 and shards % heads == 0:
            return by_features(shards, tp, tokens, w_qkv, keep_list, counts)
        return by_rows(tokens, w_qkv, keep_list, counts)

    in_specs = (P("seq", "tp"), P("seq", None, "tp"), P("seq"), P("seq"))
    out_specs = P("seq", "tp")
    return jax.shard_map(
        on_device, mesh=mesh, in_specs=in_specs, out_specs=out_specs, check_vma=False
    )
```

```python
import functools

import jax
import jax.numpy as jnp
from jax import lax
from jax.experimental import pallas as pl
from jax.experimental.pallas import tpu as pltpu
from jax.sharding import PartitionSpec as P

HD = 128


def entering(value, axis, join, neutral):
    count, mine = (lax.axis_size(axis), lax.axis_index(axis))
    pieces = lax.all_gather(value, axis)
    so_far = jnp.full_like(value, 0) + jnp.asarray(neutral, value.dtype)

    def lap(position, so_far):
        longer = join(so_far, pieces[position])
        return jnp.where(position < mine, longer, so_far)

    return lax.fori_loop(0, count - 1, lap, so_far)


def add_sums(earlier, later):
    return earlier + later


def by_rows(tokens, w_qkv, keep_list, counts):
    shards = lax.axis_size("seq")
    my_index = lax.axis_index("seq")
    tok_dev = tokens.shape[0]
    slots = keep_list.shape[0]
    capacity = slots // 2
    per_peer = slots // shards
    head_dim = HD
    columns = w_qkv.shape[2]
    local_heads = columns // head_dim
    offset = entering(counts, "seq", add_sums, jnp.zeros_like(counts))[0]
    peers = jnp.arange(shards, dtype=jnp.int32)[:, None]
    rounds = jnp.arange(per_peer, dtype=jnp.int32)[None, :]
    local_slot = (peers - offset) % shards + rounds * shards
    live = local_slot < counts[0]
    token_index = keep_list[local_slot]
    ranks = jnp.where(live, offset + local_slot, -1).astype(jnp.int32)
    positions = my_index * tok_dev + token_index
    meta = jnp.stack([positions, ranks], axis=2)
    picked = jnp.where(live[:, :, None], tokens[token_index], jnp.zeros((), tokens.dtype))
    arrived, arrived_meta = (
        lax.all_to_all(picked, "seq", split_axis=0, concat_axis=0, tiled=True),
        lax.all_to_all(meta, "seq", split_axis=0, concat_axis=0, tiled=True),
    )
    arrived_meta = arrived_meta.reshape(shards * per_peer, 2)
    arrived_rank = arrived_meta[:, 1]
    target = jnp.where(arrived_rank >= 0, arrived_rank // shards, capacity)
    flat = arrived.reshape(shards * per_peer, arrived.shape[2])
    kept = jnp.zeros((capacity, flat.shape[1]), flat.dtype).at[target].set(flat, mode="drop")
    kept_pos = jnp.zeros((capacity,), jnp.int32).at[target].set(arrived_meta[:, 0], mode="drop")
    full_rows = lax.all_gather(kept, "tp", axis=1, tiled=True)
    piece = lax.all_gather(w_qkv, "seq", axis=0, tiled=True)
    part_rows = lax.slice_in_dim(full_rows, 0, piece.shape[0], axis=1)
    projected = jnp.einsum(
        "rd,dgc->rgc", part_rows, piece, preferred_element_type=jnp.float32
    ).astype(jnp.bfloat16)
    queries = projected[:, 0].reshape(capacity, local_heads, head_dim)
    key_values = projected[:, 1:]
    scale = head_dim ** (-0.5)
    all_kv, all_pos = (
        lax.all_gather(key_values, "seq", axis=0, tiled=True),
        lax.all_gather(kept_pos, "seq", axis=0, tiled=True),
    )
    total_keys = all_kv.shape[0]
    keys_all = all_kv[:, 0].reshape(total_keys, local_heads, head_dim)
    values_all = all_kv[:, 1].reshape(total_keys, local_heads, head_dim)
    scores = (
        jnp.einsum("qhd,khd->hqk", queries, keys_all, preferred_element_type=jnp.float32) * scale
    )
    masked = all_pos[None, None, :] > kept_pos[None, :, None]
    scores = jnp.where(masked, -jnp.inf, scores)
    top = jnp.max(scores, axis=2, keepdims=True)
    expo = jnp.exp(scores - top)
    numer = jnp.einsum(
        "hqk,khd->hqd", expo.astype(jnp.bfloat16), values_all, preferred_element_type=jnp.float32
    )
    result = numer / jnp.sum(expo, axis=2)[..., None]
    return jnp.transpose(result, (1, 0, 2)).reshape(capacity, columns).astype(jnp.bfloat16)


VMEM = pl.BlockSpec(memory_space=pltpu.VMEM)
HBM = pl.BlockSpec(memory_space=pltpu.HBM)
TOP_BITS = 14


def gather(tokens, keep_list, counts):
    slots = keep_list.shape[0]
    token = lax.broadcasted_iota(jnp.int32, (tokens.shape[0], slots), 0)
    pick = (token == keep_list[None, :]).astype(jnp.bfloat16)
    rows = lax.dot_general(pick, tokens, (((0,), (0,)), ((), ())), preferred_element_type=jnp.float32)
    last = lax.broadcasted_iota(jnp.int32, rows.shape, 0) == slots - 1
    return jnp.where(last, counts[0].astype(jnp.float32), rows).astype(jnp.bfloat16)


def load_kernel(w_hbm, out_ref, sem):
    copy = pltpu.make_async_copy(w_hbm, out_ref, sem)
    copy.start()
    copy.wait()


def core_stride(shards, group):
    return shards // group if shards % group == 0 else 0


def partner(me, k, shards):
    return me ^ k if shards & (shards - 1) == 0 else (me + k) % shards


def sender(me, k, shards):
    return me ^ k if shards & (shards - 1) == 0 else (me - k + shards) % shards


def keeper(core, head, shards, heads):
    ends = [i // 2 if i % 2 == 0 else shards - 1 - i // 2 for i in range(shards)]
    return ends[(core * heads + head) % shards]


def chosen(index, options):
    value = jnp.int32(options[-1])
    for i, option in enumerate(options[:-1]):
        value = jnp.where(index == i, jnp.int32(option), value)
    return value


def own_kernel(shards, group, *refs):
    chunks, w_ref, (pick_ref, acc_ref) = refs[:shards], refs[shards], refs[shards + 1 :]
    slots, width = chunks[0].shape
    capacity = slots // 2
    kept = capacity * shards
    tp = lax.axis_index("tp")
    core = lax.rem(tp, group)
    line = lax.div(tp, group)
    stride = core_stride(shards, group)
    shard = [lax.rem(line - k - core * stride + 2 * shards, shards) for k in range(shards)]
    count = [chunks[k][slots - 1 : slots, :slots].astype(jnp.float32) for k in range(shards)]
    row = lax.broadcasted_iota(jnp.int32, (kept, slots), 0)
    rank = ((row % capacity) * shards + row // capacity).astype(jnp.float32)
    slot = lax.broadcasted_iota(jnp.int32, (kept, slots), 1).astype(jnp.float32)
    first = rank - slot
    picks = []
    for k in range(shards):
        start = jnp.zeros_like(count[k])
        for j in range(shards):
            if j != k:
                start += jnp.where(shard[j] < shard[k], count[j], 0.0)
        hit = (first == start) & (slot < count[k])
        picks.append(jnp.where(hit, 1.0, 0.0).astype(jnp.bfloat16))
        pick_ref[:, k * slots : (k + 1) * slots] = picks[k]
    rows = jnp.dot(
        jnp.concatenate(picks, axis=1),
        jnp.concatenate([chunk[...] for chunk in chunks], axis=0),
        preferred_element_type=jnp.float32,
    ).astype(jnp.bfloat16)
    where = pl.multiple_of(core * width, width)
    for kind in range(3):
        acc_ref[kind] = jnp.dot(
            rows, w_ref[kind, pl.ds(where, width), :], preferred_element_type=jnp.float32
        )


def rest_kernel(shards, group, heads, *refs):
    count = shards * (group - 1)
    halves = [refs[shards * p : shards * (p + 1)] for p in range(group - 1)]
    pick_ref, acc_ref, w_ref = refs[count : count + 3]
    outs = refs[count + 3 :]
    slots = pick_ref.shape[1] // shards
    width = w_ref.shape[1] // group
    kept = slots // 2 * shards
    stride = core_stride(shards, group)
    core = lax.rem(lax.axis_index("tp"), group)
    me = lax.axis_index("seq")
    keepers = [
        chosen(core, [keeper(c, head, shards, heads) for c in range(group)]) for head in range(heads)
    ]
    rows = []
    for p in range(1, group):
        order = [(k + p * stride) % shards for k in range(shards)]
        pick = jnp.concatenate([pick_ref[:, o * slots : (o + 1) * slots] for o in order], axis=1)
        block = jnp.concatenate([half[...] for half in halves[p - 1]], axis=0)
        rows.append(jnp.dot(pick, block, preferred_element_type=jnp.float32).astype(jnp.bfloat16))
    total = 3 * kept
    pad = outs[0].shape[0] - total
    exponents = []
    for at, kind in enumerate((1, 2, 0)):
        acc = acc_ref[kind]
        for p in range(1, group):
            where = pl.multiple_of(lax.rem(core + p, group) * width, width)
            acc += jnp.dot(
                rows[p - 1], w_ref[kind, pl.ds(where, width), :], preferred_element_type=jnp.float32
            )
        most = jnp.maximum(jnp.max(jnp.abs(acc), axis=0, keepdims=True), 2.0**-100)
        exponent = jnp.floor(jnp.log2(most)) + 1.0
        exponents.append(exponent)
        value = jnp.round(acc * jnp.exp2(TOP_BITS - exponent)).astype(jnp.int32).astype(jnp.int16)
        for k in range(shards):
            for head in range(heads):

                @pl.when(partner(me, k, shards) == keepers[head])
                def _(k=k, head=head, at=at, value=value):
                    outs[k][at * kept : (at + 1) * kept, :] = value[:, head * HD : (head + 1) * HD]

    index = lax.broadcasted_iota(jnp.int32, (pad, HD), 0)
    for head in range(heads):
        tail = jnp.zeros((pad, HD), jnp.float32)
        for at, exponent in enumerate(exponents):
            tail = jnp.where(index == at, exponent[:, head * HD : (head + 1) * HD], tail)
        tail = tail.astype(jnp.int32).astype(jnp.int16)
        for k in range(shards):

            @pl.when(partner(me, k, shards) == keepers[head])
            def _(k=k, tail=tail):
                outs[k][total:, :] = tail


def attend_kernel(shards, group, heads, *refs):
    parts, outs, all_ref = refs[:shards], refs[shards : 2 * shards], refs[2 * shards]
    kept = all_ref.shape[0]
    capacity = kept // shards
    me = lax.axis_index("seq")
    core = lax.rem(lax.axis_index("tp"), group)
    keeps = me == chosen(core, [keeper(c, 0, shards, heads) for c in range(group)])
    for head in range(1, heads):
        keeps |= me == chosen(core, [keeper(c, head, shards, heads) for c in range(group)])

    @pl.when(keeps)
    def _():
        scales = [
            jnp.exp2(p[3 * kept :, :].astype(jnp.int32).astype(jnp.float32) - TOP_BITS)
            for p in parts
        ]

        def summed(at):
            acc = None
            for p, scale in zip(parts, scales):
                part = p[at * kept : (at + 1) * kept, :].astype(jnp.int32).astype(jnp.float32)
                part = part * scale[at : at + 1, :]
                acc = part if acc is None else acc + part
            return acc.astype(jnp.bfloat16)

        key, value, query = summed(0), summed(1), summed(2)
        scores = lax.dot_general(
            query, key, (((1,), (1,)), ((), ())), preferred_element_type=jnp.float32
        ) * (HD ** (-0.5))
        q_row = lax.broadcasted_iota(jnp.int32, scores.shape, 0)
        k_row = lax.broadcasted_iota(jnp.int32, scores.shape, 1)
        q_rank = lax.rem(q_row, capacity) * shards + lax.div(q_row, capacity)
        k_rank = lax.rem(k_row, capacity) * shards + lax.div(k_row, capacity)
        scores = jnp.where(k_rank > q_rank, -jnp.inf, scores)
        top = jnp.max(scores, axis=1, keepdims=True)
        expo = jnp.exp(scores - top)
        numer = jnp.dot(expo.astype(jnp.bfloat16), value, preferred_element_type=jnp.float32)
        all_ref[...] = numer / jnp.sum(expo, axis=1, keepdims=True)
        for k in range(shards):
            owner = pl.multiple_of(partner(me, k, shards) * capacity, capacity)
            outs[k][...] = all_ref[pl.ds(owner, capacity), :].astype(jnp.bfloat16)


def by_features(shards, tp, tokens, w_qkv, keep_list, counts):
    group = tp // shards
    slots = keep_list.shape[0]
    capacity = slots // 2
    kept = capacity * shards
    heads = w_qkv.shape[2] // HD
    axes = ("seq", "tp")
    params = pltpu.CompilerParams(vmem_limit_bytes=32 * 1024 * 1024)

    def device(s, line, core):
        return s * tp + line * group + core

    packed = gather(tokens, keep_list, counts)
    stride = core_stride(shards, group)
    every = [(s, line, c) for s in range(shards) for line in range(shards) for c in range(group)]
    own = []
    for k in range(shards):
        pairs = [
            (device(s, line, c), device(line, (s + k + c * stride) % shards, c))
            for s, line, c in every
        ]
        own.append(lax.ppermute(packed, axes, pairs))
    others = []
    for p in range(1, group):
        pairs = [
            (line * group + (c + p) % group, line * group + c)
            for line in range(shards)
            for c in range(group)
        ]
        for k in range(shards):
            others.append(lax.ppermute(own[k], "tp", pairs))
    weights = jnp.transpose(w_qkv, (1, 0, 2))
    weights = pl.pallas_call(
        load_kernel,
        out_shape=jax.ShapeDtypeStruct(weights.shape, weights.dtype),
        in_specs=[HBM],
        out_specs=VMEM,
        scratch_shapes=[pltpu.SemaphoreType.DMA],
        compiler_params=pltpu.CompilerParams(vmem_limit_bytes=51 * 1024 * 1024),
        name="load",
    )(weights)
    pick, acc = pl.pallas_call(
        functools.partial(own_kernel, shards, group),
        out_shape=[
            jax.ShapeDtypeStruct((kept, shards * slots), jnp.bfloat16),
            jax.ShapeDtypeStruct((3, kept, heads * HD), jnp.float32),
        ],
        in_specs=[VMEM] * (shards + 1),
        out_specs=[VMEM] * 2,
        compiler_params=params,
        name="own",
    )(*own, weights)
    payload = 3 * kept + 16
    partial = pl.pallas_call(
        functools.partial(rest_kernel, shards, group, heads),
        out_shape=[jax.ShapeDtypeStruct((payload, HD), jnp.int16)] * shards,
        in_specs=[VMEM] * (shards * (group - 1) + 3),
        out_specs=[VMEM] * shards,
        compiler_params=params,
        name="rest",
    )(*others, pick, acc, weights)
    keepers = [[keeper(c, head, shards, heads) for head in range(heads)] for c in range(group)]
    parts = [partial[0]]
    for k in range(1, shards):
        pairs = [
            (device(sender(d, k, shards), line, c), device(d, line, c))
            for line in range(shards)
            for c in range(group)
            for d in keepers[c]
        ]
        parts.append(lax.ppermute(partial[k], axes, pairs))
    pieces = pl.pallas_call(
        functools.partial(attend_kernel, shards, group, heads),
        out_shape=[jax.ShapeDtypeStruct((capacity, HD), jnp.bfloat16)] * shards,
        in_specs=[VMEM] * shards,
        out_specs=[VMEM] * shards,
        scratch_shapes=[pltpu.VMEM((kept, HD), jnp.float32)],
        compiler_params=params,
        name="attend",
    )(*parts)
    arrived = [pieces[0]]
    for k in range(1, shards):
        pairs = [
            (device(d, line, c), device(partner(d, k, shards), line, c))
            for line in range(shards)
            for c in range(group)
            for d in keepers[c]
        ]
        arrived.append(lax.ppermute(pieces[k], axes, pairs))
    mine = lax.axis_index("seq")
    core = lax.rem(lax.axis_index("tp"), group)
    columns = []
    for head in range(heads):
        source = chosen(core, [keepers[c][head] for c in range(group)])
        column = arrived[0]
        for k in range(1, shards):
            column = jnp.where(sender(mine, k, shards) == source, arrived[k], column)
        columns.append(column)
    return jnp.concatenate(columns, axis=1)


def fits(mesh):
    shards, tp = mesh.shape["seq"], mesh.shape["tp"]
    return tp % shards == 0 and tp > shards


def solution(mesh):
    shards, tp = mesh.shape["seq"], mesh.shape["tp"]

    def on_device(tokens, w_qkv, keep_list, counts):
        heads = w_qkv.shape[2] // HD
        if fits(mesh) and shards >= heads:
            return by_features(shards, tp, tokens, w_qkv, keep_list, counts)
        return by_rows(tokens, w_qkv, keep_list, counts)

    in_specs = (P("seq", "tp"), P("seq", None, "tp"), P("seq"), P("seq"))
    out_specs = P("seq", "tp")
    return jax.shard_map(
        on_device, mesh=mesh, in_specs=in_specs, out_specs=out_specs, check_vma=False
    )
```

```python
import functools

import jax
import jax.numpy as jnp
from jax import lax
from jax.experimental import pallas as pl
from jax.experimental.pallas import tpu as pltpu
from jax.sharding import PartitionSpec as P

HD = 128


def entering(value, axis, join, neutral):
    count, mine = (lax.axis_size(axis), lax.axis_index(axis))
    pieces = lax.all_gather(value, axis)
    so_far = jnp.full_like(value, 0) + jnp.asarray(neutral, value.dtype)

    def lap(position, so_far):
        longer = join(so_far, pieces[position])
        return jnp.where(position < mine, longer, so_far)

    return lax.fori_loop(0, count - 1, lap, so_far)


def add_sums(earlier, later):
    return earlier + later


def by_rows(tokens, w_qkv, keep_list, counts):
    shards = lax.axis_size("seq")
    my_index = lax.axis_index("seq")
    tok_dev = tokens.shape[0]
    slots = keep_list.shape[0]
    capacity = slots // 2
    per_peer = slots // shards
    head_dim = HD
    columns = w_qkv.shape[2]
    local_heads = columns // head_dim
    offset = entering(counts, "seq", add_sums, jnp.zeros_like(counts))[0]
    peers = jnp.arange(shards, dtype=jnp.int32)[:, None]
    rounds = jnp.arange(per_peer, dtype=jnp.int32)[None, :]
    local_slot = (peers - offset) % shards + rounds * shards
    live = local_slot < counts[0]
    token_index = keep_list[local_slot]
    ranks = jnp.where(live, offset + local_slot, -1).astype(jnp.int32)
    positions = my_index * tok_dev + token_index
    meta = jnp.stack([positions, ranks], axis=2)
    picked = jnp.where(live[:, :, None], tokens[token_index], jnp.zeros((), tokens.dtype))
    arrived, arrived_meta = (
        lax.all_to_all(picked, "seq", split_axis=0, concat_axis=0, tiled=True),
        lax.all_to_all(meta, "seq", split_axis=0, concat_axis=0, tiled=True),
    )
    arrived_meta = arrived_meta.reshape(shards * per_peer, 2)
    arrived_rank = arrived_meta[:, 1]
    target = jnp.where(arrived_rank >= 0, arrived_rank // shards, capacity)
    flat = arrived.reshape(shards * per_peer, arrived.shape[2])
    kept = jnp.zeros((capacity, flat.shape[1]), flat.dtype).at[target].set(flat, mode="drop")
    kept_pos = jnp.zeros((capacity,), jnp.int32).at[target].set(arrived_meta[:, 0], mode="drop")
    full_rows = lax.all_gather(kept, "tp", axis=1, tiled=True)
    piece = lax.all_gather(w_qkv, "seq", axis=0, tiled=True)
    part_rows = lax.slice_in_dim(full_rows, 0, piece.shape[0], axis=1)
    projected = jnp.einsum(
        "rd,dgc->rgc", part_rows, piece, preferred_element_type=jnp.float32
    ).astype(jnp.bfloat16)
    queries = projected[:, 0].reshape(capacity, local_heads, head_dim)
    key_values = projected[:, 1:]
    scale = head_dim ** (-0.5)
    all_kv, all_pos = (
        lax.all_gather(key_values, "seq", axis=0, tiled=True),
        lax.all_gather(kept_pos, "seq", axis=0, tiled=True),
    )
    total_keys = all_kv.shape[0]
    keys_all = all_kv[:, 0].reshape(total_keys, local_heads, head_dim)
    values_all = all_kv[:, 1].reshape(total_keys, local_heads, head_dim)
    scores = (
        jnp.einsum("qhd,khd->hqk", queries, keys_all, preferred_element_type=jnp.float32) * scale
    )
    masked = all_pos[None, None, :] > kept_pos[None, :, None]
    scores = jnp.where(masked, -jnp.inf, scores)
    top = jnp.max(scores, axis=2, keepdims=True)
    expo = jnp.exp(scores - top)
    numer = jnp.einsum(
        "hqk,khd->hqd", expo.astype(jnp.bfloat16), values_all, preferred_element_type=jnp.float32
    )
    result = numer / jnp.sum(expo, axis=2)[..., None]
    return jnp.transpose(result, (1, 0, 2)).reshape(capacity, columns).astype(jnp.bfloat16)


VMEM = pl.BlockSpec(memory_space=pltpu.VMEM)
HBM = pl.BlockSpec(memory_space=pltpu.HBM)
TOP_BITS = 14


def gather(tokens, keep_list, counts):
    slots = keep_list.shape[0]
    token = lax.broadcasted_iota(jnp.int32, (tokens.shape[0], slots), 0)
    pick = (token == keep_list[None, :]).astype(jnp.bfloat16)
    rows = lax.dot_general(pick, tokens, (((0,), (0,)), ((), ())), preferred_element_type=jnp.float32)
    last = lax.broadcasted_iota(jnp.int32, rows.shape, 0) == slots - 1
    return jnp.where(last, counts[0].astype(jnp.float32), rows).astype(jnp.bfloat16)


def load_kernel(w_hbm, out_ref, sem):
    copy = pltpu.make_async_copy(w_hbm, out_ref, sem)
    copy.start()
    copy.wait()


def core_stride(shards, group):
    return shards // group if shards % group == 0 else 0


def own_kernel(shards, group, *refs):
    chunks, w_ref, (pick_ref, acc_ref) = refs[:shards], refs[shards], refs[shards + 1 :]
    slots, width = chunks[0].shape
    capacity = slots // 2
    kept = capacity * shards
    tp = lax.axis_index("tp")
    core = lax.rem(tp, group)
    line = lax.div(tp, group)
    stride = core_stride(shards, group)
    shard = [lax.rem(line - k - core * stride + 2 * shards, shards) for k in range(shards)]
    count = [chunks[k][slots - 1 : slots, :slots].astype(jnp.float32) for k in range(shards)]
    row = lax.broadcasted_iota(jnp.int32, (kept, slots), 0)
    rank = ((row % capacity) * shards + row // capacity).astype(jnp.float32)
    slot = lax.broadcasted_iota(jnp.int32, (kept, slots), 1).astype(jnp.float32)
    first = rank - slot
    picks = []
    for k in range(shards):
        start = jnp.zeros_like(count[k])
        for j in range(shards):
            if j != k:
                start += jnp.where(shard[j] < shard[k], count[j], 0.0)
        hit = (first == start) & (slot < count[k])
        picks.append(jnp.where(hit, 1.0, 0.0).astype(jnp.bfloat16))
        pick_ref[:, k * slots : (k + 1) * slots] = picks[k]
    rows = jnp.dot(
        jnp.concatenate(picks, axis=1),
        jnp.concatenate([chunk[...] for chunk in chunks], axis=0),
        preferred_element_type=jnp.float32,
    ).astype(jnp.bfloat16)
    where = pl.multiple_of(core * width, width)
    for kind in range(3):
        acc_ref[kind] = jnp.dot(
            rows, w_ref[kind, pl.ds(where, width), :], preferred_element_type=jnp.float32
        )


def rest_kernel(shards, group, heads, *refs):
    count = shards * (group - 1)
    halves = [refs[shards * p : shards * (p + 1)] for p in range(group - 1)]
    pick_ref, acc_ref, w_ref = refs[count : count + 3]
    outs = refs[count + 3 :]
    slots = pick_ref.shape[1] // shards
    width = w_ref.shape[1] // group
    kept = slots // 2 * shards
    blocks = shards // heads
    block_rows = kept // blocks
    stride = core_stride(shards, group)
    core = lax.rem(lax.axis_index("tp"), group)
    me = lax.axis_index("seq")
    rows = []
    for p in range(1, group):
        order = [(k + p * stride) % shards for k in range(shards)]
        pick = jnp.concatenate([pick_ref[:, o * slots : (o + 1) * slots] for o in order], axis=1)
        block = jnp.concatenate([half[...] for half in halves[p - 1]], axis=0)
        rows.append(jnp.dot(pick, block, preferred_element_type=jnp.float32).astype(jnp.bfloat16))
    total = 2 * kept + block_rows
    pad = outs[0].shape[0] - total
    exponents = []
    for at, kind in enumerate((1, 2, 0)):
        acc = acc_ref[kind]
        for p in range(1, group):
            where = pl.multiple_of(lax.rem(core + p, group) * width, width)
            acc += jnp.dot(
                rows[p - 1], w_ref[kind, pl.ds(where, width), :], preferred_element_type=jnp.float32
            )
        most = jnp.maximum(jnp.max(jnp.abs(acc), axis=0, keepdims=True), 2.0**-100)
        exponent = jnp.floor(jnp.log2(most)) + 1.0
        exponents.append(exponent)
        value = jnp.round(acc * jnp.exp2(TOP_BITS - exponent)).astype(jnp.int32).astype(jnp.int16)
        for k in range(shards):
            dest = lax.rem(me + k, shards)
            for head in range(heads):
                mine = value[:, head * HD : (head + 1) * HD]
                if kind:

                    @pl.when(lax.rem(dest, heads) == head)
                    def _(k=k, at=at, mine=mine):
                        outs[k][at * kept : (at + 1) * kept, :] = mine
                else:
                    for b in range(blocks):

                        @pl.when(dest == b * heads + head)
                        def _(k=k, b=b, mine=mine):
                            outs[k][2 * kept : total, :] = mine[b * block_rows : (b + 1) * block_rows, :]

    index = lax.broadcasted_iota(jnp.int32, (pad, HD), 0)
    for head in range(heads):
        tail = jnp.zeros((pad, HD), jnp.float32)
        for at, exponent in enumerate(exponents):
            tail = jnp.where(index == at, exponent[:, head * HD : (head + 1) * HD], tail)
        tail = tail.astype(jnp.int32).astype(jnp.int16)
        for k in range(shards):

            @pl.when(lax.rem(lax.rem(me + k, shards), heads) == head)
            def _(k=k, tail=tail):
                outs[k][total:, :] = tail


def attend_kernel(shards, heads, kept, *refs):
    parts, outs = refs[:shards], refs[shards:]
    capacity = kept // shards
    me = lax.axis_index("seq")
    block_rows = kept // (shards // heads)
    total = 2 * kept + block_rows
    block = lax.div(me, heads)
    scales = [
        jnp.exp2(p[total:, :].astype(jnp.int32).astype(jnp.float32) - TOP_BITS) for p in parts
    ]

    def summed(i, lo, hi):
        acc = None
        for p, scale in zip(parts, scales):
            part = p[lo:hi, :].astype(jnp.int32).astype(jnp.float32) * scale[i : i + 1, :]
            acc = part if acc is None else acc + part
        return acc.astype(jnp.bfloat16)

    key, value, query = summed(0, 0, kept), summed(1, kept, 2 * kept), summed(2, 2 * kept, total)
    scores = lax.dot_general(
        query, key, (((1,), (1,)), ((), ())), preferred_element_type=jnp.float32
    ) * (HD ** (-0.5))
    q_row = lax.broadcasted_iota(jnp.int32, scores.shape, 0) + block * block_rows
    k_row = lax.broadcasted_iota(jnp.int32, scores.shape, 1)
    q_rank = lax.rem(q_row, capacity) * shards + lax.div(q_row, capacity)
    k_rank = lax.rem(k_row, capacity) * shards + lax.div(k_row, capacity)
    scores = jnp.where(k_rank > q_rank, -jnp.inf, scores)
    top = jnp.max(scores, axis=1, keepdims=True)
    expo = jnp.exp(scores - top)
    numer = jnp.dot(expo.astype(jnp.bfloat16), value, preferred_element_type=jnp.float32)
    result = (numer / jnp.sum(expo, axis=1, keepdims=True)).astype(jnp.bfloat16)
    head = lax.rem(me, heads)
    for k in range(heads):
        owner = lax.rem(head + k, heads)
        for o in range(heads):

            @pl.when(owner == o)
            def _(k=k, o=o):
                outs[k][...] = result[o * capacity : (o + 1) * capacity, :]


def by_features(shards, tp, tokens, w_qkv, keep_list, counts):
    group = tp // shards
    slots = keep_list.shape[0]
    capacity = slots // 2
    kept = capacity * shards
    heads = w_qkv.shape[2] // HD
    axes = ("seq", "tp")
    params = pltpu.CompilerParams(vmem_limit_bytes=32 * 1024 * 1024)

    def device(s, line, core):
        return s * tp + line * group + core

    packed = gather(tokens, keep_list, counts)
    stride = core_stride(shards, group)
    every = [(s, line, c) for s in range(shards) for line in range(shards) for c in range(group)]
    own = []
    for k in range(shards):
        pairs = [
            (device(s, line, c), device(line, (s + k + c * stride) % shards, c))
            for s, line, c in every
        ]
        own.append(lax.ppermute(packed, axes, pairs))
    others = []
    for p in range(1, group):
        pairs = [
            (line * group + (c + p) % group, line * group + c)
            for line in range(shards)
            for c in range(group)
        ]
        for k in range(shards):
            others.append(lax.ppermute(own[k], "tp", pairs))
    weights = jnp.transpose(w_qkv, (1, 0, 2))
    weights = pl.pallas_call(
        load_kernel,
        out_shape=jax.ShapeDtypeStruct(weights.shape, weights.dtype),
        in_specs=[HBM],
        out_specs=VMEM,
        scratch_shapes=[pltpu.SemaphoreType.DMA],
        compiler_params=pltpu.CompilerParams(vmem_limit_bytes=51 * 1024 * 1024),
        name="load",
    )(weights)
    pick, acc = pl.pallas_call(
        functools.partial(own_kernel, shards, group),
        out_shape=[
            jax.ShapeDtypeStruct((kept, shards * slots), jnp.bfloat16),
            jax.ShapeDtypeStruct((3, kept, heads * HD), jnp.float32),
        ],
        in_specs=[VMEM] * (shards + 1),
        out_specs=[VMEM] * 2,
        compiler_params=params,
        name="own",
    )(*own, weights)
    blocks = shards // heads
    payload = 2 * kept + kept // blocks + 16
    partial = pl.pallas_call(
        functools.partial(rest_kernel, shards, group, heads),
        out_shape=[jax.ShapeDtypeStruct((payload, HD), jnp.int16)] * shards,
        in_specs=[VMEM] * (shards * (group - 1) + 3),
        out_specs=[VMEM] * shards,
        compiler_params=params,
        name="rest",
    )(*others, pick, acc, weights)
    parts = [partial[0]]
    for k in range(1, shards):
        pairs = [(s, (s + k) % shards) for s in range(shards)]
        parts.append(lax.ppermute(partial[k], "seq", pairs))
    pieces = pl.pallas_call(
        functools.partial(attend_kernel, shards, heads, kept),
        out_shape=[jax.ShapeDtypeStruct((capacity, HD), jnp.bfloat16)] * heads,
        in_specs=[VMEM] * shards,
        out_specs=[VMEM] * heads,
        compiler_params=params,
        name="attend",
    )(*parts)
    arrived = [pieces[0]]
    for k in range(1, heads):
        pairs = [
            (b * heads + h, b * heads + (h + k) % heads) for b in range(blocks) for h in range(heads)
        ]
        arrived.append(lax.ppermute(pieces[k], "seq", pairs))
    mine = lax.rem(lax.axis_index("seq"), heads)
    columns = []
    for h in range(heads):
        column = arrived[0]
        for k in range(1, heads):
            column = jnp.where(lax.rem(mine - k + heads, heads) == h, arrived[k], column)
        columns.append(column)
    return jnp.concatenate(columns, axis=1)


def fits(mesh):
    shards, tp = mesh.shape["seq"], mesh.shape["tp"]
    return tp % shards == 0 and tp > shards


def solution(mesh):
    shards, tp = mesh.shape["seq"], mesh.shape["tp"]

    def on_device(tokens, w_qkv, keep_list, counts):
        heads = w_qkv.shape[2] // HD
        if fits(mesh) and shards % heads == 0:
            return by_features(shards, tp, tokens, w_qkv, keep_list, counts)
        return by_rows(tokens, w_qkv, keep_list, counts)

    in_specs = (P("seq", "tp"), P("seq", None, "tp"), P("seq"), P("seq"))
    out_specs = P("seq", "tp")
    return jax.shard_map(
        on_device, mesh=mesh, in_specs=in_specs, out_specs=out_specs, check_vma=False
    )
```

```python
import functools

import jax
import jax.numpy as jnp
from jax import lax
from jax.experimental import pallas as pl
from jax.experimental.pallas import tpu as pltpu
from jax.sharding import PartitionSpec as P

HD = 128


def entering(value, axis, join, neutral):
    count, mine = (lax.axis_size(axis), lax.axis_index(axis))
    pieces = lax.all_gather(value, axis)
    so_far = jnp.full_like(value, 0) + jnp.asarray(neutral, value.dtype)

    def lap(position, so_far):
        longer = join(so_far, pieces[position])
        return jnp.where(position < mine, longer, so_far)

    return lax.fori_loop(0, count - 1, lap, so_far)


def add_sums(earlier, later):
    return earlier + later


def by_rows(tokens, w_qkv, keep_list, counts):
    shards = lax.axis_size("seq")
    my_index = lax.axis_index("seq")
    tok_dev = tokens.shape[0]
    slots = keep_list.shape[0]
    capacity = slots // 2
    per_peer = slots // shards
    head_dim = HD
    columns = w_qkv.shape[2]
    local_heads = columns // head_dim
    offset = entering(counts, "seq", add_sums, jnp.zeros_like(counts))[0]
    peers = jnp.arange(shards, dtype=jnp.int32)[:, None]
    rounds = jnp.arange(per_peer, dtype=jnp.int32)[None, :]
    local_slot = (peers - offset) % shards + rounds * shards
    live = local_slot < counts[0]
    token_index = keep_list[local_slot]
    ranks = jnp.where(live, offset + local_slot, -1).astype(jnp.int32)
    positions = my_index * tok_dev + token_index
    meta = jnp.stack([positions, ranks], axis=2)
    picked = jnp.where(live[:, :, None], tokens[token_index], jnp.zeros((), tokens.dtype))
    arrived, arrived_meta = (
        lax.all_to_all(picked, "seq", split_axis=0, concat_axis=0, tiled=True),
        lax.all_to_all(meta, "seq", split_axis=0, concat_axis=0, tiled=True),
    )
    arrived_meta = arrived_meta.reshape(shards * per_peer, 2)
    arrived_rank = arrived_meta[:, 1]
    target = jnp.where(arrived_rank >= 0, arrived_rank // shards, capacity)
    flat = arrived.reshape(shards * per_peer, arrived.shape[2])
    kept = jnp.zeros((capacity, flat.shape[1]), flat.dtype).at[target].set(flat, mode="drop")
    kept_pos = jnp.zeros((capacity,), jnp.int32).at[target].set(arrived_meta[:, 0], mode="drop")
    full_rows = lax.all_gather(kept, "tp", axis=1, tiled=True)
    piece = lax.all_gather(w_qkv, "seq", axis=0, tiled=True)
    part_rows = lax.slice_in_dim(full_rows, 0, piece.shape[0], axis=1)
    projected = jnp.einsum(
        "rd,dgc->rgc", part_rows, piece, preferred_element_type=jnp.float32
    ).astype(jnp.bfloat16)
    queries = projected[:, 0].reshape(capacity, local_heads, head_dim)
    key_values = projected[:, 1:]
    scale = head_dim ** (-0.5)
    all_kv, all_pos = (
        lax.all_gather(key_values, "seq", axis=0, tiled=True),
        lax.all_gather(kept_pos, "seq", axis=0, tiled=True),
    )
    total_keys = all_kv.shape[0]
    keys_all = all_kv[:, 0].reshape(total_keys, local_heads, head_dim)
    values_all = all_kv[:, 1].reshape(total_keys, local_heads, head_dim)
    scores = (
        jnp.einsum("qhd,khd->hqk", queries, keys_all, preferred_element_type=jnp.float32) * scale
    )
    masked = all_pos[None, None, :] > kept_pos[None, :, None]
    scores = jnp.where(masked, -jnp.inf, scores)
    top = jnp.max(scores, axis=2, keepdims=True)
    expo = jnp.exp(scores - top)
    numer = jnp.einsum(
        "hqk,khd->hqd", expo.astype(jnp.bfloat16), values_all, preferred_element_type=jnp.float32
    )
    result = numer / jnp.sum(expo, axis=2)[..., None]
    return jnp.transpose(result, (1, 0, 2)).reshape(capacity, columns).astype(jnp.bfloat16)


VMEM = pl.BlockSpec(memory_space=pltpu.VMEM)
HBM = pl.BlockSpec(memory_space=pltpu.HBM)
TOP_BITS = 14
CORES = 2
FIRST = 2


def gather_kernel(counts_ref, keep_ref, tokens_ref, pick_ref, out_ref):
    slots = out_ref.shape[0]
    token = lax.broadcasted_iota(jnp.int32, (tokens_ref.shape[0], slots), 0)
    pick = (token == keep_ref[...]).astype(jnp.bfloat16)
    pick_ref[...] = pick
    rows = lax.dot_general(
        pick, tokens_ref[...], (((0,), (0,)), ((), ())), preferred_element_type=jnp.float32
    )
    count = counts_ref[0].astype(jnp.float32)
    last = lax.broadcasted_iota(jnp.int32, rows.shape, 0) == slots - 1
    out_ref[...] = jnp.where(last, count, rows).astype(jnp.bfloat16)


def join_kernel(pick_ref, own_ref, other_ref, out_ref):
    slots = own_ref.shape[0]
    rows = lax.dot_general(
        pick_ref[...], other_ref[...], (((0,), (0,)), ((), ())), preferred_element_type=jnp.float32
    )
    last = lax.broadcasted_iota(jnp.int32, rows.shape, 0) == slots - 1
    count = own_ref[slots - 1 : slots, :].astype(jnp.float32)
    out_ref[:slots, :] = own_ref[...]
    out_ref[slots:, :] = jnp.where(last, count, rows).astype(jnp.bfloat16)


def load_kernel(w_hbm, out_ref, sem):
    copy = pltpu.make_async_copy(w_hbm, out_ref, sem)
    copy.start()
    copy.wait()


def early_kernel(shards, *refs):
    ops = shards // CORES
    chunks, w_ref, (pick_ref, acc_ref) = refs[: shards - 1], refs[shards - 1], refs[shards:]
    slots, width = pick_ref.shape[1], chunks[0].shape[1]
    kept = pick_ref.shape[0]
    capacity = kept // shards
    tp = lax.axis_index("tp")
    core = lax.rem(tp, CORES)
    line = lax.div(tp, CORES)
    own_shard = [lax.rem(line - shift(k, core, shards) + 4 * shards, shards) for k in range(ops)]
    shard = own_shard + [lax.rem(o + ops, shards) for o in own_shard]
    count = [chunk[slots - 1 : slots, :slots].astype(jnp.float32) for chunk in chunks]
    count.append(kept - functools.reduce(lambda x, y: x + y, count))
    row = lax.broadcasted_iota(jnp.int32, (kept, slots), 0)
    rank = ((row % capacity) * shards + row // capacity).astype(jnp.float32)
    slot = lax.broadcasted_iota(jnp.int32, (kept, slots), 1).astype(jnp.float32)
    first = rank - slot
    picks = []
    for k in range(shards):
        start = jnp.zeros_like(count[k])
        for j in range(shards):
            if j != k:
                start += jnp.where(shard[j] < shard[k], count[j], 0.0)
        hit = (first == start) & (slot < count[k])
        picks.append(jnp.where(hit, 1.0, 0.0).astype(jnp.bfloat16))
    pick_ref[...] = picks[-1]
    pick = jnp.concatenate(picks[:-1], axis=1)
    rows = []
    for q in range(CORES):
        block = jnp.concatenate(
            [
                chunk[at * slots : (at + 1) * slots, :]
                for chunk, at in zip(chunks, [q] * ops + [1 - q] * (ops - 1))
            ],
            axis=0,
        )
        rows.append(jnp.dot(pick, block, preferred_element_type=jnp.float32).astype(jnp.bfloat16))
    for kind in range(3):
        acc_ref[kind] = times(rows, w_ref, kind, core, width)


def times(rows, w_ref, kind, core, width):
    acc = None
    for q in range(CORES):
        where = pl.multiple_of(lax.rem(core + q, CORES) * width, width)
        part = jnp.dot(
            rows[q], w_ref[kind, pl.ds(where, width), :], preferred_element_type=jnp.float32
        )
        acc = part if acc is None else acc + part
    return acc


def rest_kernel(shards, heads, chunk_ref, pick_ref, acc_ref, w_ref, *outs):
    kept, slots = pick_ref.shape
    width = chunk_ref.shape[1]
    blocks = shards // heads
    block_rows = kept // blocks
    core = lax.rem(lax.axis_index("tp"), CORES)
    me = lax.axis_index("seq")
    rows = [
        jnp.dot(
            pick_ref[...],
            chunk_ref[(1 - q) * slots : (2 - q) * slots, :],
            preferred_element_type=jnp.float32,
        ).astype(jnp.bfloat16)
        for q in range(CORES)
    ]
    total = 2 * kept + block_rows
    pad = outs[0].shape[0] - total
    exponents = []
    for at, kind in enumerate((1, 2, 0)):
        acc = acc_ref[kind] + times(rows, w_ref, kind, core, width)
        most = jnp.maximum(jnp.max(jnp.abs(acc), axis=0, keepdims=True), 2.0**-100)
        exponent = jnp.floor(jnp.log2(most)) + 1.0
        exponents.append(exponent)
        value = jnp.round(acc * jnp.exp2(TOP_BITS - exponent)).astype(jnp.int32).astype(jnp.int16)
        for k in range(shards):
            dest = lax.rem(me + k, shards)
            for head in range(heads):
                mine = value[:, head * HD : (head + 1) * HD]
                if kind:

                    @pl.when(lax.rem(dest, heads) == head)
                    def _(k=k, at=at, mine=mine):
                        outs[k][at * kept : (at + 1) * kept, :] = mine
                else:
                    for b in range(blocks):

                        @pl.when(dest == b * heads + head)
                        def _(k=k, b=b, mine=mine):
                            outs[k][2 * kept : total, :] = mine[b * block_rows : (b + 1) * block_rows, :]

    index = lax.broadcasted_iota(jnp.int32, (pad, HD), 0)
    for head in range(heads):
        tail = jnp.zeros((pad, HD), jnp.float32)
        for at, exponent in enumerate(exponents):
            tail = jnp.where(index == at, exponent[:, head * HD : (head + 1) * HD], tail)
        tail = tail.astype(jnp.int32).astype(jnp.int16)
        for k in range(shards):

            @pl.when(lax.rem(lax.rem(me + k, shards), heads) == head)
            def _(k=k, tail=tail):
                outs[k][total:, :] = tail


def attend_kernel(shards, heads, kept, *refs):
    parts, outs = refs[:shards], refs[shards:]
    capacity = kept // shards
    me = lax.axis_index("seq")
    block_rows = kept // (shards // heads)
    total = 2 * kept + block_rows
    block = lax.div(me, heads)
    scales = [
        jnp.exp2(p[total:, :].astype(jnp.int32).astype(jnp.float32) - TOP_BITS) for p in parts
    ]

    def summed(i, lo, hi):
        acc = None
        for p, scale in zip(parts, scales):
            part = p[lo:hi, :].astype(jnp.int32).astype(jnp.float32) * scale[i : i + 1, :]
            acc = part if acc is None else acc + part
        return acc.astype(jnp.bfloat16)

    key, value, query = summed(0, 0, kept), summed(1, kept, 2 * kept), summed(2, 2 * kept, total)
    scores = lax.dot_general(
        query, key, (((1,), (1,)), ((), ())), preferred_element_type=jnp.float32
    ) * (HD ** (-0.5))
    q_row = lax.broadcasted_iota(jnp.int32, scores.shape, 0) + block * block_rows
    k_row = lax.broadcasted_iota(jnp.int32, scores.shape, 1)
    q_rank = lax.rem(q_row, capacity) * shards + lax.div(q_row, capacity)
    k_rank = lax.rem(k_row, capacity) * shards + lax.div(k_row, capacity)
    scores = jnp.where(k_rank > q_rank, -jnp.inf, scores)
    top = jnp.max(scores, axis=1, keepdims=True)
    expo = jnp.exp(scores - top)
    numer = jnp.dot(expo.astype(jnp.bfloat16), value, preferred_element_type=jnp.float32)
    result = (numer / jnp.sum(expo, axis=1, keepdims=True)).astype(jnp.bfloat16)
    head = lax.rem(me, heads)
    for k in range(heads):
        owner = lax.rem(head + k, heads)
        for o in range(heads):

            @pl.when(owner == o)
            def _(k=k, o=o):
                outs[k][...] = result[o * capacity : (o + 1) * capacity, :]


def shift(k, core, shards):
    return FIRST + k + core * (shards // CORES)


def by_features(shards, tokens, w_qkv, keep_list, counts):
    tp = shards * CORES
    slots = keep_list.shape[0]
    capacity = slots // 2
    kept = capacity * shards
    width = tokens.shape[1]
    heads = w_qkv.shape[2] // HD
    ops = shards // CORES
    params = pltpu.CompilerParams(vmem_limit_bytes=32 * 1024 * 1024)

    def device(s, line, core):
        return s * tp + line * CORES + core

    swap = [(line * CORES + c, line * CORES + 1 - c) for line in range(shards) for c in range(CORES)]
    other = lax.ppermute(tokens, "tp", swap)
    pick, mine = pl.pallas_call(
        gather_kernel,
        out_shape=[
            jax.ShapeDtypeStruct((tokens.shape[0], slots), jnp.bfloat16),
            jax.ShapeDtypeStruct((slots, width), jnp.bfloat16),
        ],
        in_specs=[pl.BlockSpec(memory_space=pltpu.SMEM), VMEM, VMEM],
        out_specs=[VMEM] * 2,
        compiler_params=params,
        name="gather",
    )(counts, keep_list.reshape(1, slots), tokens)
    packed = pl.pallas_call(
        join_kernel,
        out_shape=jax.ShapeDtypeStruct((CORES * slots, width), jnp.bfloat16),
        in_specs=[VMEM] * 3,
        out_specs=VMEM,
        compiler_params=params,
        name="join",
    )(pick, mine, other)
    every = [(s, line, c) for s in range(shards) for line in range(shards) for c in range(CORES)]
    own = []
    for k in range(ops):
        pairs = [
            (device(s, line, c), device(line, (s + shift(k, c, shards)) % shards, c))
            for s, line, c in every
        ]
        own.append(lax.ppermute(packed, ("seq", "tp"), pairs))
    others = []
    for k in range(ops):
        others.append(lax.ppermute(own[k], "tp", swap))
    weights = jnp.transpose(w_qkv, (1, 0, 2))
    weights = pl.pallas_call(
        load_kernel,
        out_shape=jax.ShapeDtypeStruct(weights.shape, weights.dtype),
        in_specs=[HBM],
        out_specs=VMEM,
        scratch_shapes=[pltpu.SemaphoreType.DMA],
        compiler_params=pltpu.CompilerParams(vmem_limit_bytes=51 * 1024 * 1024),
        name="load",
    )(weights)
    pick, acc = pl.pallas_call(
        functools.partial(early_kernel, shards),
        out_shape=[
            jax.ShapeDtypeStruct((kept, slots), jnp.bfloat16),
            jax.ShapeDtypeStruct((3, kept, heads * HD), jnp.float32),
        ],
        in_specs=[VMEM] * shards,
        out_specs=[VMEM] * 2,
        compiler_params=params,
        name="early",
    )(*own, *others[:-1], weights)
    blocks = shards // heads
    payload = 2 * kept + kept // blocks + 16
    partial = pl.pallas_call(
        functools.partial(rest_kernel, shards, heads),
        out_shape=[jax.ShapeDtypeStruct((payload, HD), jnp.int16)] * shards,
        in_specs=[VMEM] * 4,
        out_specs=[VMEM] * shards,
        compiler_params=params,
        name="rest",
    )(others[-1], pick, acc, weights)
    parts = [partial[0]]
    for k in range(1, shards):
        pairs = [(s, (s + k) % shards) for s in range(shards)]
        parts.append(lax.ppermute(partial[k], "seq", pairs))
    pieces = pl.pallas_call(
        functools.partial(attend_kernel, shards, heads, kept),
        out_shape=[jax.ShapeDtypeStruct((capacity, HD), jnp.bfloat16)] * heads,
        in_specs=[VMEM] * shards,
        out_specs=[VMEM] * heads,
        compiler_params=params,
        name="attend",
    )(*parts)
    arrived = [pieces[0]]
    for k in range(1, heads):
        pairs = [
            (b * heads + h, b * heads + (h + k) % heads) for b in range(blocks) for h in range(heads)
        ]
        arrived.append(lax.ppermute(pieces[k], "seq", pairs))
    mine = lax.rem(lax.axis_index("seq"), heads)
    columns = []
    for h in range(heads):
        column = arrived[0]
        for k in range(1, heads):
            column = jnp.where(lax.rem(mine - k + heads, heads) == h, arrived[k], column)
        columns.append(column)
    return jnp.concatenate(columns, axis=1)


def fits(mesh):
    shards, tp = mesh.shape["seq"], mesh.shape["tp"]
    return tp == shards * CORES and shards % CORES == 0


def solution(mesh):
    shards = mesh.shape["seq"]

    def on_device(tokens, w_qkv, keep_list, counts):
        heads = w_qkv.shape[2] // HD
        if fits(mesh) and shards % heads == 0:
            return by_features(shards, tokens, w_qkv, keep_list, counts)
        return by_rows(tokens, w_qkv, keep_list, counts)

    in_specs = (P("seq", "tp"), P("seq", None, "tp"), P("seq"), P("seq"))
    out_specs = P("seq", "tp")
    return jax.shard_map(
        on_device, mesh=mesh, in_specs=in_specs, out_specs=out_specs, check_vma=False
    )
```

```python
import functools

import jax
import jax.numpy as jnp
from jax import lax
from jax.experimental import pallas as pl
from jax.experimental.pallas import tpu as pltpu
from jax.sharding import PartitionSpec as P

HD = 128


def entering(value, axis, join, neutral):
    count, mine = (lax.axis_size(axis), lax.axis_index(axis))
    pieces = lax.all_gather(value, axis)
    so_far = jnp.full_like(value, 0) + jnp.asarray(neutral, value.dtype)

    def lap(position, so_far):
        longer = join(so_far, pieces[position])
        return jnp.where(position < mine, longer, so_far)

    return lax.fori_loop(0, count - 1, lap, so_far)


def add_sums(earlier, later):
    return earlier + later


def by_rows(tokens, w_qkv, keep_list, counts):
    shards = lax.axis_size("seq")
    my_index = lax.axis_index("seq")
    tok_dev = tokens.shape[0]
    slots = keep_list.shape[0]
    capacity = slots // 2
    per_peer = slots // shards
    head_dim = HD
    columns = w_qkv.shape[2]
    local_heads = columns // head_dim
    offset = entering(counts, "seq", add_sums, jnp.zeros_like(counts))[0]
    peers = jnp.arange(shards, dtype=jnp.int32)[:, None]
    rounds = jnp.arange(per_peer, dtype=jnp.int32)[None, :]
    local_slot = (peers - offset) % shards + rounds * shards
    live = local_slot < counts[0]
    token_index = keep_list[local_slot]
    ranks = jnp.where(live, offset + local_slot, -1).astype(jnp.int32)
    positions = my_index * tok_dev + token_index
    meta = jnp.stack([positions, ranks], axis=2)
    picked = jnp.where(live[:, :, None], tokens[token_index], jnp.zeros((), tokens.dtype))
    arrived, arrived_meta = (
        lax.all_to_all(picked, "seq", split_axis=0, concat_axis=0, tiled=True),
        lax.all_to_all(meta, "seq", split_axis=0, concat_axis=0, tiled=True),
    )
    arrived_meta = arrived_meta.reshape(shards * per_peer, 2)
    arrived_rank = arrived_meta[:, 1]
    target = jnp.where(arrived_rank >= 0, arrived_rank // shards, capacity)
    flat = arrived.reshape(shards * per_peer, arrived.shape[2])
    kept = jnp.zeros((capacity, flat.shape[1]), flat.dtype).at[target].set(flat, mode="drop")
    kept_pos = jnp.zeros((capacity,), jnp.int32).at[target].set(arrived_meta[:, 0], mode="drop")
    full_rows = lax.all_gather(kept, "tp", axis=1, tiled=True)
    piece = lax.all_gather(w_qkv, "seq", axis=0, tiled=True)
    part_rows = lax.slice_in_dim(full_rows, 0, piece.shape[0], axis=1)
    projected = jnp.einsum(
        "rd,dgc->rgc", part_rows, piece, preferred_element_type=jnp.float32
    ).astype(jnp.bfloat16)
    queries = projected[:, 0].reshape(capacity, local_heads, head_dim)
    key_values = projected[:, 1:]
    scale = head_dim ** (-0.5)
    all_kv, all_pos = (
        lax.all_gather(key_values, "seq", axis=0, tiled=True),
        lax.all_gather(kept_pos, "seq", axis=0, tiled=True),
    )
    total_keys = all_kv.shape[0]
    keys_all = all_kv[:, 0].reshape(total_keys, local_heads, head_dim)
    values_all = all_kv[:, 1].reshape(total_keys, local_heads, head_dim)
    scores = (
        jnp.einsum("qhd,khd->hqk", queries, keys_all, preferred_element_type=jnp.float32) * scale
    )
    masked = all_pos[None, None, :] > kept_pos[None, :, None]
    scores = jnp.where(masked, -jnp.inf, scores)
    top = jnp.max(scores, axis=2, keepdims=True)
    expo = jnp.exp(scores - top)
    numer = jnp.einsum(
        "hqk,khd->hqd", expo.astype(jnp.bfloat16), values_all, preferred_element_type=jnp.float32
    )
    result = numer / jnp.sum(expo, axis=2)[..., None]
    return jnp.transpose(result, (1, 0, 2)).reshape(capacity, columns).astype(jnp.bfloat16)


VMEM = pl.BlockSpec(memory_space=pltpu.VMEM)
HBM = pl.BlockSpec(memory_space=pltpu.HBM)
TOP_BITS = 14


def gather(tokens, keep_list, counts):
    slots = keep_list.shape[0]
    token = lax.broadcasted_iota(jnp.int32, (tokens.shape[0], slots), 0)
    pick = lax.optimization_barrier((token == keep_list[None, :]).astype(jnp.bfloat16))
    rows = lax.dot_general(pick, tokens, (((0,), (0,)), ((), ())), preferred_element_type=jnp.float32)
    last = lax.broadcasted_iota(jnp.int32, rows.shape, 0) == slots - 1
    return jnp.where(last, counts[0].astype(jnp.float32), rows).astype(jnp.bfloat16)


def load_kernel(w_hbm, out_ref, sem):
    copy = pltpu.make_async_copy(w_hbm, out_ref, sem)
    copy.start()
    copy.wait()


def core_stride(shards, group):
    return shards // group if shards % group == 0 else 0


def own_kernel(shards, group, *refs):
    chunks, w_ref, (pick_ref, acc_ref) = refs[:shards], refs[shards], refs[shards + 1 :]
    slots, width = chunks[0].shape
    capacity = slots // 2
    kept = capacity * shards
    tp = lax.axis_index("tp")
    core = lax.rem(tp, group)
    line = lax.div(tp, group)
    stride = core_stride(shards, group)
    shard = [lax.rem(k + core * stride - line + shards, shards) for k in range(shards)]
    count = [chunks[k][slots - 1 : slots, :slots].astype(jnp.float32) for k in range(shards)]
    row = lax.broadcasted_iota(jnp.int32, (kept, slots), 0)
    rank = ((row % capacity) * shards + row // capacity).astype(jnp.float32)
    slot = lax.broadcasted_iota(jnp.int32, (kept, slots), 1).astype(jnp.float32)
    first = rank - slot
    picks = []
    for k in range(shards):
        start = jnp.zeros_like(count[k])
        for j in range(shards):
            if j != k:
                start += jnp.where(shard[j] < shard[k], count[j], 0.0)
        hit = (first == start) & (slot < count[k])
        picks.append(jnp.where(hit, 1.0, 0.0).astype(jnp.bfloat16))
        pick_ref[:, k * slots : (k + 1) * slots] = picks[k]
    rows = jnp.dot(
        jnp.concatenate(picks, axis=1),
        jnp.concatenate([chunk[...] for chunk in chunks], axis=0),
        preferred_element_type=jnp.float32,
    ).astype(jnp.bfloat16)
    where = pl.multiple_of(core * width, width)
    for kind in range(3):
        acc_ref[kind] = jnp.dot(
            rows, w_ref[kind, pl.ds(where, width), :], preferred_element_type=jnp.float32
        )


def rest_kernel(shards, group, heads, *refs):
    count = shards * (group - 1)
    halves = [refs[shards * p : shards * (p + 1)] for p in range(group - 1)]
    pick_ref, acc_ref, w_ref = refs[count : count + 3]
    outs = refs[count + 3 :]
    slots = pick_ref.shape[1] // shards
    width = w_ref.shape[1] // group
    kept = slots // 2 * shards
    blocks = shards // heads
    block_rows = kept // blocks
    stride = core_stride(shards, group)
    core = lax.rem(lax.axis_index("tp"), group)
    me = lax.axis_index("seq")
    rows = []
    for p in range(1, group):
        order = [(k + p * stride) % shards for k in range(shards)]
        pick = jnp.concatenate([pick_ref[:, o * slots : (o + 1) * slots] for o in order], axis=1)
        block = jnp.concatenate([half[...] for half in halves[p - 1]], axis=0)
        rows.append(jnp.dot(pick, block, preferred_element_type=jnp.float32).astype(jnp.bfloat16))
    total = 2 * kept + block_rows
    pad = outs[0].shape[0] - total
    exponents = []
    for at, kind in enumerate((1, 2, 0)):
        acc = acc_ref[kind]
        for p in range(1, group):
            where = pl.multiple_of(lax.rem(core + p, group) * width, width)
            acc += jnp.dot(
                rows[p - 1], w_ref[kind, pl.ds(where, width), :], preferred_element_type=jnp.float32
            )
        most = jnp.maximum(jnp.max(jnp.abs(acc), axis=0, keepdims=True), 2.0**-100)
        exponent = jnp.floor(jnp.log2(most)) + 1.0
        exponents.append(exponent)
        value = jnp.round(acc * jnp.exp2(TOP_BITS - exponent)).astype(jnp.int32)
        for r in range(heads):
            mine = of_head(value, lax.rem(me + r, heads), heads)
            if kind:
                mine = mine.astype(jnp.int16)
                for k in range(r, shards, heads):
                    outs[k][at * kept : (at + 1) * kept, :] = mine
            else:
                for k in range(r, shards, heads):
                    block = lax.div(lax.rem(me + k, shards), heads)
                    part = mine[:block_rows, :]
                    for b in range(1, blocks):
                        part = jnp.where(block == b, mine[b * block_rows : (b + 1) * block_rows, :], part)
                    outs[k][2 * kept : total, :] = part.astype(jnp.int16)

    index = lax.broadcasted_iota(jnp.int32, (pad, heads * HD), 0)
    tail = jnp.zeros((pad, heads * HD), jnp.float32)
    for at, exponent in enumerate(exponents):
        tail = jnp.where(index == at, exponent, tail)
    tail = tail.astype(jnp.int32)
    for r in range(heads):
        mine = of_head(tail, lax.rem(me + r, heads), heads).astype(jnp.int16)
        for k in range(r, shards, heads):
            outs[k][total:, :] = mine


def of_head(value, head, heads):
    mine = value[:, :HD]
    for h in range(1, heads):
        mine = jnp.where(head == h, value[:, h * HD : (h + 1) * HD], mine)
    return mine


def attend_kernel(shards, heads, kept, *refs):
    parts, outs = refs[:shards], refs[shards:]
    capacity = kept // shards
    me = lax.axis_index("seq")
    block_rows = kept // (shards // heads)
    total = 2 * kept + block_rows
    block = lax.div(me, heads)
    scales = [
        jnp.exp2(p[total:, :].astype(jnp.int32).astype(jnp.float32) - TOP_BITS) for p in parts
    ]

    def summed(i, lo, hi):
        acc = None
        for p, scale in zip(parts, scales):
            part = p[lo:hi, :].astype(jnp.int32).astype(jnp.float32) * scale[i : i + 1, :]
            acc = part if acc is None else acc + part
        return acc.astype(jnp.bfloat16)

    key, value, query = summed(0, 0, kept), summed(1, kept, 2 * kept), summed(2, 2 * kept, total)
    scores = lax.dot_general(
        query, key, (((1,), (1,)), ((), ())), preferred_element_type=jnp.float32
    ) * (HD ** (-0.5))
    q_row = lax.broadcasted_iota(jnp.int32, scores.shape, 0) + block * block_rows
    k_row = lax.broadcasted_iota(jnp.int32, scores.shape, 1)
    q_rank = lax.rem(q_row, capacity) * shards + lax.div(q_row, capacity)
    k_rank = lax.rem(k_row, capacity) * shards + lax.div(k_row, capacity)
    scores = jnp.where(k_rank > q_rank, -jnp.inf, scores)
    top = jnp.max(scores, axis=1, keepdims=True)
    expo = jnp.exp(scores - top)
    numer = jnp.dot(expo.astype(jnp.bfloat16), value, preferred_element_type=jnp.float32)
    result = numer / jnp.sum(expo, axis=1, keepdims=True)
    head = lax.rem(me, heads)
    for k in range(heads):
        owner = lax.rem(head + k, heads)
        piece = result[:capacity, :]
        for o in range(1, heads):
            piece = jnp.where(owner == o, result[o * capacity : (o + 1) * capacity, :], piece)
        outs[k][...] = piece.astype(jnp.bfloat16)


def by_features(shards, tp, tokens, w_qkv, keep_list, counts):
    group = tp // shards
    slots = keep_list.shape[0]
    capacity = slots // 2
    kept = capacity * shards
    heads = w_qkv.shape[2] // HD
    axes = ("seq", "tp")
    params = pltpu.CompilerParams(vmem_limit_bytes=32 * 1024 * 1024)

    def device(s, line, core):
        return s * tp + line * group + core

    packed = gather(tokens, keep_list, counts)
    stride = core_stride(shards, group)
    every = [(s, line, c) for s in range(shards) for line in range(shards) for c in range(group)]
    own = []
    for k in range(shards):
        pairs = [
            (device(s, line, c), device(line, (k + c * stride - s) % shards, c))
            for s, line, c in every
        ]
        own.append(lax.ppermute(packed, axes, pairs))
    others = []
    for p in range(1, group):
        pairs = [
            (line * group + (c + p) % group, line * group + c)
            for line in range(shards)
            for c in range(group)
        ]
        for k in range(shards):
            others.append(lax.ppermute(own[k], "tp", pairs))
    weights = jnp.transpose(w_qkv, (1, 0, 2))
    weights = pl.pallas_call(
        load_kernel,
        out_shape=jax.ShapeDtypeStruct(weights.shape, weights.dtype),
        in_specs=[HBM],
        out_specs=VMEM,
        scratch_shapes=[pltpu.SemaphoreType.DMA],
        compiler_params=pltpu.CompilerParams(vmem_limit_bytes=51 * 1024 * 1024),
        name="load",
    )(weights)
    pick, acc = pl.pallas_call(
        functools.partial(own_kernel, shards, group),
        out_shape=[
            jax.ShapeDtypeStruct((kept, shards * slots), jnp.bfloat16),
            jax.ShapeDtypeStruct((3, kept, heads * HD), jnp.float32),
        ],
        in_specs=[VMEM] * (shards + 1),
        out_specs=[VMEM] * 2,
        compiler_params=params,
        name="own",
    )(*own, weights)
    blocks = shards // heads
    payload = 2 * kept + kept // blocks + 16
    partial = pl.pallas_call(
        functools.partial(rest_kernel, shards, group, heads),
        out_shape=[jax.ShapeDtypeStruct((payload, HD), jnp.int16)] * shards,
        in_specs=[VMEM] * (shards * (group - 1) + 3),
        out_specs=[VMEM] * shards,
        compiler_params=params,
        name="rest",
    )(*others, pick, acc, weights)
    parts = [partial[0]]
    for k in range(1, shards):
        pairs = [(s, (s + k) % shards) for s in range(shards)]
        parts.append(lax.ppermute(partial[k], "seq", pairs))
    pieces = pl.pallas_call(
        functools.partial(attend_kernel, shards, heads, kept),
        out_shape=[jax.ShapeDtypeStruct((capacity, HD), jnp.bfloat16)] * heads,
        in_specs=[VMEM] * shards,
        out_specs=[VMEM] * heads,
        compiler_params=params,
        name="attend",
    )(*parts)
    arrived = [pieces[0]]
    for k in range(1, heads):
        pairs = [
            (b * heads + h, b * heads + (h + k) % heads) for b in range(blocks) for h in range(heads)
        ]
        arrived.append(lax.ppermute(pieces[k], "seq", pairs))
    mine = lax.rem(lax.axis_index("seq"), heads)
    columns = []
    for h in range(heads):
        column = arrived[0]
        for k in range(1, heads):
            column = jnp.where(lax.rem(mine - k + heads, heads) == h, arrived[k], column)
        columns.append(column)
    return jnp.concatenate(columns, axis=1)


def fits(mesh):
    shards, tp = mesh.shape["seq"], mesh.shape["tp"]
    return tp % shards == 0 and tp > shards


def solution(mesh):
    shards, tp = mesh.shape["seq"], mesh.shape["tp"]

    def on_device(tokens, w_qkv, keep_list, counts):
        heads = w_qkv.shape[2] // HD
        if fits(mesh) and shards % heads == 0:
            return by_features(shards, tp, tokens, w_qkv, keep_list, counts)
        return by_rows(tokens, w_qkv, keep_list, counts)

    in_specs = (P("seq", "tp"), P("seq", None, "tp"), P("seq"), P("seq"))
    out_specs = P("seq", "tp")
    return jax.shard_map(
        on_device, mesh=mesh, in_specs=in_specs, out_specs=out_specs, check_vma=False
    )
```

```python
import functools

import jax
import jax.numpy as jnp
from jax import lax
from jax.experimental import pallas as pl
from jax.experimental.pallas import tpu as pltpu
from jax.sharding import PartitionSpec as P

HD = 128


def entering(value, axis, join, neutral):
    count, mine = (lax.axis_size(axis), lax.axis_index(axis))
    pieces = lax.all_gather(value, axis)
    so_far = jnp.full_like(value, 0) + jnp.asarray(neutral, value.dtype)

    def lap(position, so_far):
        longer = join(so_far, pieces[position])
        return jnp.where(position < mine, longer, so_far)

    return lax.fori_loop(0, count - 1, lap, so_far)


def add_sums(earlier, later):
    return earlier + later


def by_rows(tokens, w_qkv, keep_list, counts):
    shards = lax.axis_size("seq")
    my_index = lax.axis_index("seq")
    tok_dev = tokens.shape[0]
    slots = keep_list.shape[0]
    capacity = slots // 2
    per_peer = slots // shards
    head_dim = HD
    columns = w_qkv.shape[2]
    local_heads = columns // head_dim
    offset = entering(counts, "seq", add_sums, jnp.zeros_like(counts))[0]
    peers = jnp.arange(shards, dtype=jnp.int32)[:, None]
    rounds = jnp.arange(per_peer, dtype=jnp.int32)[None, :]
    local_slot = (peers - offset) % shards + rounds * shards
    live = local_slot < counts[0]
    token_index = keep_list[local_slot]
    ranks = jnp.where(live, offset + local_slot, -1).astype(jnp.int32)
    positions = my_index * tok_dev + token_index
    meta = jnp.stack([positions, ranks], axis=2)
    picked = jnp.where(live[:, :, None], tokens[token_index], jnp.zeros((), tokens.dtype))
    arrived, arrived_meta = (
        lax.all_to_all(picked, "seq", split_axis=0, concat_axis=0, tiled=True),
        lax.all_to_all(meta, "seq", split_axis=0, concat_axis=0, tiled=True),
    )
    arrived_meta = arrived_meta.reshape(shards * per_peer, 2)
    arrived_rank = arrived_meta[:, 1]
    target = jnp.where(arrived_rank >= 0, arrived_rank // shards, capacity)
    flat = arrived.reshape(shards * per_peer, arrived.shape[2])
    kept = jnp.zeros((capacity, flat.shape[1]), flat.dtype).at[target].set(flat, mode="drop")
    kept_pos = jnp.zeros((capacity,), jnp.int32).at[target].set(arrived_meta[:, 0], mode="drop")
    full_rows = lax.all_gather(kept, "tp", axis=1, tiled=True)
    piece = lax.all_gather(w_qkv, "seq", axis=0, tiled=True)
    part_rows = lax.slice_in_dim(full_rows, 0, piece.shape[0], axis=1)
    projected = jnp.einsum(
        "rd,dgc->rgc", part_rows, piece, preferred_element_type=jnp.float32
    ).astype(jnp.bfloat16)
    queries = projected[:, 0].reshape(capacity, local_heads, head_dim)
    key_values = projected[:, 1:]
    scale = head_dim ** (-0.5)
    all_kv, all_pos = (
        lax.all_gather(key_values, "seq", axis=0, tiled=True),
        lax.all_gather(kept_pos, "seq", axis=0, tiled=True),
    )
    total_keys = all_kv.shape[0]
    keys_all = all_kv[:, 0].reshape(total_keys, local_heads, head_dim)
    values_all = all_kv[:, 1].reshape(total_keys, local_heads, head_dim)
    scores = (
        jnp.einsum("qhd,khd->hqk", queries, keys_all, preferred_element_type=jnp.float32) * scale
    )
    masked = all_pos[None, None, :] > kept_pos[None, :, None]
    scores = jnp.where(masked, -jnp.inf, scores)
    top = jnp.max(scores, axis=2, keepdims=True)
    expo = jnp.exp(scores - top)
    numer = jnp.einsum(
        "hqk,khd->hqd", expo.astype(jnp.bfloat16), values_all, preferred_element_type=jnp.float32
    )
    result = numer / jnp.sum(expo, axis=2)[..., None]
    return jnp.transpose(result, (1, 0, 2)).reshape(capacity, columns).astype(jnp.bfloat16)


VMEM = pl.BlockSpec(memory_space=pltpu.VMEM)
HBM = pl.BlockSpec(memory_space=pltpu.HBM)
TOP_BITS = 14


def gather(tokens, keep_list, counts):
    slots = keep_list.shape[0]
    token = lax.broadcasted_iota(jnp.int32, (tokens.shape[0], slots), 0)
    pick = lax.optimization_barrier((token == keep_list[None, :]).astype(jnp.bfloat16))
    rows = lax.dot_general(pick, tokens, (((0,), (0,)), ((), ())), preferred_element_type=jnp.float32)
    last = lax.broadcasted_iota(jnp.int32, rows.shape, 0) == slots - 1
    return jnp.where(last, counts[0].astype(jnp.float32), rows).astype(jnp.bfloat16)


def load_kernel(w_hbm, out_ref, sem):
    copy = pltpu.make_async_copy(w_hbm, out_ref, sem)
    copy.start()
    copy.wait()


def core_stride(shards, group):
    return shards // group if shards % group == 0 else 0


def toward(me, k, shards):
    return me ^ k if shards & (shards - 1) == 0 else (me + k) % shards


def step(j, core, shards):
    return shards - j if j and core % 2 else j


def own_kernel(shards, group, *refs):
    chunks, w_ref, (pick_ref, acc_ref) = refs[:shards], refs[shards], refs[shards + 1 :]
    slots, width = chunks[0].shape
    capacity = slots // 2
    kept = capacity * shards
    tp = lax.axis_index("tp")
    core = lax.rem(tp, group)
    line = lax.div(tp, group)
    stride = core_stride(shards, group)
    shard = [lax.rem(k + core * stride - line + shards, shards) for k in range(shards)]
    count = [chunks[k][slots - 1 : slots, :slots].astype(jnp.float32) for k in range(shards)]
    row = lax.broadcasted_iota(jnp.int32, (kept, slots), 0)
    rank = ((row % capacity) * shards + row // capacity).astype(jnp.float32)
    slot = lax.broadcasted_iota(jnp.int32, (kept, slots), 1).astype(jnp.float32)
    first = rank - slot
    picks = []
    for k in range(shards):
        start = jnp.zeros_like(count[k])
        for j in range(shards):
            if j != k:
                start += jnp.where(shard[j] < shard[k], count[j], 0.0)
        hit = (first == start) & (slot < count[k])
        picks.append(jnp.where(hit, 1.0, 0.0).astype(jnp.bfloat16))
        pick_ref[:, k * slots : (k + 1) * slots] = picks[k]
    rows = jnp.dot(
        jnp.concatenate(picks, axis=1),
        jnp.concatenate([chunk[...] for chunk in chunks], axis=0),
        preferred_element_type=jnp.float32,
    ).astype(jnp.bfloat16)
    where = pl.multiple_of(core * width, width)
    for kind in range(3):
        acc_ref[kind] = jnp.dot(
            rows, w_ref[kind, pl.ds(where, width), :], preferred_element_type=jnp.float32
        )


def rest_kernel(shards, group, heads, *refs):
    count = shards * (group - 1)
    halves = [refs[shards * p : shards * (p + 1)] for p in range(group - 1)]
    pick_ref, acc_ref, w_ref = refs[count : count + 3]
    outs = refs[count + 3 :]
    slots = pick_ref.shape[1] // shards
    width = w_ref.shape[1] // group
    kept = slots // 2 * shards
    blocks = shards // heads
    block_rows = kept // blocks
    stride = core_stride(shards, group)
    core = lax.rem(lax.axis_index("tp"), group)
    me = lax.axis_index("seq")
    rows = []
    for p in range(1, group):
        order = [(k + p * stride) % shards for k in range(shards)]
        pick = jnp.concatenate([pick_ref[:, o * slots : (o + 1) * slots] for o in order], axis=1)
        block = jnp.concatenate([half[...] for half in halves[p - 1]], axis=0)
        rows.append(jnp.dot(pick, block, preferred_element_type=jnp.float32).astype(jnp.bfloat16))
    total = 2 * kept + block_rows
    pad = outs[0].shape[0] - total
    dests = [me]
    for k in range(1, shards):
        dest = toward(me, step(k, 0, shards), shards)
        for c in range(1, group):
            dest = jnp.where(core == c, toward(me, step(k, c, shards), shards), dest)
        dests.append(dest)
    exponents = []
    for at, kind in enumerate((1, 2, 0)):
        acc = acc_ref[kind]
        for p in range(1, group):
            where = pl.multiple_of(lax.rem(core + p, group) * width, width)
            acc += jnp.dot(
                rows[p - 1], w_ref[kind, pl.ds(where, width), :], preferred_element_type=jnp.float32
            )
        most = jnp.maximum(jnp.max(jnp.abs(acc), axis=0, keepdims=True), 2.0**-100)
        exponent = jnp.floor(jnp.log2(most)) + 1.0
        exponents.append(exponent)
        value = jnp.round(acc * jnp.exp2(TOP_BITS - exponent)).astype(jnp.int32)
        for k, dest in enumerate(dests):
            mine = of_head(value, lax.rem(dest, heads), heads)
            if kind:
                outs[k][at * kept : (at + 1) * kept, :] = mine.astype(jnp.int16)
            else:
                block = lax.div(dest, heads)
                part = mine[:block_rows, :]
                for b in range(1, blocks):
                    part = jnp.where(block == b, mine[b * block_rows : (b + 1) * block_rows, :], part)
                outs[k][2 * kept : total, :] = part.astype(jnp.int16)

    index = lax.broadcasted_iota(jnp.int32, (pad, heads * HD), 0)
    tail = jnp.zeros((pad, heads * HD), jnp.float32)
    for at, exponent in enumerate(exponents):
        tail = jnp.where(index == at, exponent, tail)
    tail = tail.astype(jnp.int32)
    for k, dest in enumerate(dests):
        outs[k][total:, :] = of_head(tail, lax.rem(dest, heads), heads).astype(jnp.int16)


def of_head(value, head, heads):
    mine = value[:, :HD]
    for h in range(1, heads):
        mine = jnp.where(head == h, value[:, h * HD : (h + 1) * HD], mine)
    return mine


def attend_kernel(shards, heads, kept, *refs):
    parts, outs = refs[:shards], refs[shards:]
    capacity = kept // shards
    me = lax.axis_index("seq")
    block_rows = kept // (shards // heads)
    total = 2 * kept + block_rows
    block = lax.div(me, heads)
    scales = [
        jnp.exp2(p[total:, :].astype(jnp.int32).astype(jnp.float32) - TOP_BITS) for p in parts
    ]

    def summed(i, lo, hi):
        acc = None
        for p, scale in zip(parts, scales):
            part = p[lo:hi, :].astype(jnp.int32).astype(jnp.float32) * scale[i : i + 1, :]
            acc = part if acc is None else acc + part
        return acc.astype(jnp.bfloat16)

    key, value, query = summed(0, 0, kept), summed(1, kept, 2 * kept), summed(2, 2 * kept, total)
    scores = lax.dot_general(
        query, key, (((1,), (1,)), ((), ())), preferred_element_type=jnp.float32
    ) * (HD ** (-0.5))
    q_row = lax.broadcasted_iota(jnp.int32, scores.shape, 0) + block * block_rows
    k_row = lax.broadcasted_iota(jnp.int32, scores.shape, 1)
    q_rank = lax.rem(q_row, capacity) * shards + lax.div(q_row, capacity)
    k_rank = lax.rem(k_row, capacity) * shards + lax.div(k_row, capacity)
    scores = jnp.where(k_rank > q_rank, -jnp.inf, scores)
    top = jnp.max(scores, axis=1, keepdims=True)
    expo = jnp.exp(scores - top)
    numer = jnp.dot(expo.astype(jnp.bfloat16), value, preferred_element_type=jnp.float32)
    result = numer / jnp.sum(expo, axis=1, keepdims=True)
    head = lax.rem(me, heads)
    for k in range(heads):
        owner = lax.rem(head + k, heads)
        piece = result[:capacity, :]
        for o in range(1, heads):
            piece = jnp.where(owner == o, result[o * capacity : (o + 1) * capacity, :], piece)
        outs[k][...] = piece.astype(jnp.bfloat16)


def by_features(shards, tp, tokens, w_qkv, keep_list, counts):
    group = tp // shards
    slots = keep_list.shape[0]
    capacity = slots // 2
    kept = capacity * shards
    heads = w_qkv.shape[2] // HD
    axes = ("seq", "tp")
    params = pltpu.CompilerParams(vmem_limit_bytes=32 * 1024 * 1024)

    def device(s, line, core):
        return s * tp + line * group + core

    packed = gather(tokens, keep_list, counts)
    stride = core_stride(shards, group)
    every = [(s, line, c) for s in range(shards) for line in range(shards) for c in range(group)]
    own = []
    for k in range(shards):
        pairs = [
            (device(s, line, c), device(line, (k + c * stride - s) % shards, c))
            for s, line, c in every
        ]
        own.append(lax.ppermute(packed, axes, pairs))
    others = []
    for p in range(1, group):
        pairs = [
            (line * group + (c + p) % group, line * group + c)
            for line in range(shards)
            for c in range(group)
        ]
        for k in range(shards):
            others.append(lax.ppermute(own[k], "tp", pairs))
    weights = jnp.transpose(w_qkv, (1, 0, 2))
    weights = pl.pallas_call(
        load_kernel,
        out_shape=jax.ShapeDtypeStruct(weights.shape, weights.dtype),
        in_specs=[HBM],
        out_specs=VMEM,
        scratch_shapes=[pltpu.SemaphoreType.DMA],
        compiler_params=pltpu.CompilerParams(vmem_limit_bytes=51 * 1024 * 1024),
        name="load",
    )(weights)
    pick, acc = pl.pallas_call(
        functools.partial(own_kernel, shards, group),
        out_shape=[
            jax.ShapeDtypeStruct((kept, shards * slots), jnp.bfloat16),
            jax.ShapeDtypeStruct((3, kept, heads * HD), jnp.float32),
        ],
        in_specs=[VMEM] * (shards + 1),
        out_specs=[VMEM] * 2,
        compiler_params=params,
        name="own",
    )(*own, weights)
    blocks = shards // heads
    payload = 2 * kept + kept // blocks + 16
    partial = pl.pallas_call(
        functools.partial(rest_kernel, shards, group, heads),
        out_shape=[jax.ShapeDtypeStruct((payload, HD), jnp.int16)] * shards,
        in_specs=[VMEM] * (shards * (group - 1) + 3),
        out_specs=[VMEM] * shards,
        compiler_params=params,
        name="rest",
    )(*others, pick, acc, weights)
    parts = [partial[0]]
    for k in range(1, shards):
        pairs = [
            (device(s, line, c), device(toward(s, step(k, c, shards), shards), line, c))
            for s, line, c in every
        ]
        parts.append(lax.ppermute(partial[k], ("seq", "tp"), pairs))
    pieces = pl.pallas_call(
        functools.partial(attend_kernel, shards, heads, kept),
        out_shape=[jax.ShapeDtypeStruct((capacity, HD), jnp.bfloat16)] * heads,
        in_specs=[VMEM] * shards,
        out_specs=[VMEM] * heads,
        compiler_params=params,
        name="attend",
    )(*parts)
    arrived = [pieces[0]]
    for k in range(1, heads):
        pairs = [
            (b * heads + h, b * heads + (h + k) % heads) for b in range(blocks) for h in range(heads)
        ]
        arrived.append(lax.ppermute(pieces[k], "seq", pairs))
    mine = lax.rem(lax.axis_index("seq"), heads)
    columns = []
    for h in range(heads):
        column = arrived[0]
        for k in range(1, heads):
            column = jnp.where(lax.rem(mine - k + heads, heads) == h, arrived[k], column)
        columns.append(column)
    return jnp.concatenate(columns, axis=1)


def fits(mesh):
    shards, tp = mesh.shape["seq"], mesh.shape["tp"]
    return tp % shards == 0 and tp > shards


def solution(mesh):
    shards, tp = mesh.shape["seq"], mesh.shape["tp"]

    def on_device(tokens, w_qkv, keep_list, counts):
        heads = w_qkv.shape[2] // HD
        if fits(mesh) and shards % heads == 0:
            return by_features(shards, tp, tokens, w_qkv, keep_list, counts)
        return by_rows(tokens, w_qkv, keep_list, counts)

    in_specs = (P("seq", "tp"), P("seq", None, "tp"), P("seq"), P("seq"))
    out_specs = P("seq", "tp")
    return jax.shard_map(
        on_device, mesh=mesh, in_specs=in_specs, out_specs=out_specs, check_vma=False
    )
```

```python
import functools

import jax
import jax.numpy as jnp
from jax import lax
from jax.experimental import pallas as pl
from jax.experimental.pallas import tpu as pltpu
from jax.sharding import PartitionSpec as P

HD = 128


def entering(value, axis, join, neutral):
    count, mine = (lax.axis_size(axis), lax.axis_index(axis))
    pieces = lax.all_gather(value, axis)
    so_far = jnp.full_like(value, 0) + jnp.asarray(neutral, value.dtype)

    def lap(position, so_far):
        longer = join(so_far, pieces[position])
        return jnp.where(position < mine, longer, so_far)

    return lax.fori_loop(0, count - 1, lap, so_far)


def add_sums(earlier, later):
    return earlier + later


def by_rows(tokens, w_qkv, keep_list, counts):
    shards = lax.axis_size("seq")
    my_index = lax.axis_index("seq")
    tok_dev = tokens.shape[0]
    slots = keep_list.shape[0]
    capacity = slots // 2
    per_peer = slots // shards
    head_dim = HD
    columns = w_qkv.shape[2]
    local_heads = columns // head_dim
    offset = entering(counts, "seq", add_sums, jnp.zeros_like(counts))[0]
    peers = jnp.arange(shards, dtype=jnp.int32)[:, None]
    rounds = jnp.arange(per_peer, dtype=jnp.int32)[None, :]
    local_slot = (peers - offset) % shards + rounds * shards
    live = local_slot < counts[0]
    token_index = keep_list[local_slot]
    ranks = jnp.where(live, offset + local_slot, -1).astype(jnp.int32)
    positions = my_index * tok_dev + token_index
    meta = jnp.stack([positions, ranks], axis=2)
    picked = jnp.where(live[:, :, None], tokens[token_index], jnp.zeros((), tokens.dtype))
    arrived, arrived_meta = (
        lax.all_to_all(picked, "seq", split_axis=0, concat_axis=0, tiled=True),
        lax.all_to_all(meta, "seq", split_axis=0, concat_axis=0, tiled=True),
    )
    arrived_meta = arrived_meta.reshape(shards * per_peer, 2)
    arrived_rank = arrived_meta[:, 1]
    target = jnp.where(arrived_rank >= 0, arrived_rank // shards, capacity)
    flat = arrived.reshape(shards * per_peer, arrived.shape[2])
    kept = jnp.zeros((capacity, flat.shape[1]), flat.dtype).at[target].set(flat, mode="drop")
    kept_pos = jnp.zeros((capacity,), jnp.int32).at[target].set(arrived_meta[:, 0], mode="drop")
    full_rows = lax.all_gather(kept, "tp", axis=1, tiled=True)
    piece = lax.all_gather(w_qkv, "seq", axis=0, tiled=True)
    part_rows = lax.slice_in_dim(full_rows, 0, piece.shape[0], axis=1)
    projected = jnp.einsum(
        "rd,dgc->rgc", part_rows, piece, preferred_element_type=jnp.float32
    ).astype(jnp.bfloat16)
    queries = projected[:, 0].reshape(capacity, local_heads, head_dim)
    key_values = projected[:, 1:]
    scale = head_dim ** (-0.5)
    all_kv, all_pos = (
        lax.all_gather(key_values, "seq", axis=0, tiled=True),
        lax.all_gather(kept_pos, "seq", axis=0, tiled=True),
    )
    total_keys = all_kv.shape[0]
    keys_all = all_kv[:, 0].reshape(total_keys, local_heads, head_dim)
    values_all = all_kv[:, 1].reshape(total_keys, local_heads, head_dim)
    scores = (
        jnp.einsum("qhd,khd->hqk", queries, keys_all, preferred_element_type=jnp.float32) * scale
    )
    masked = all_pos[None, None, :] > kept_pos[None, :, None]
    scores = jnp.where(masked, -jnp.inf, scores)
    top = jnp.max(scores, axis=2, keepdims=True)
    expo = jnp.exp(scores - top)
    numer = jnp.einsum(
        "hqk,khd->hqd", expo.astype(jnp.bfloat16), values_all, preferred_element_type=jnp.float32
    )
    result = numer / jnp.sum(expo, axis=2)[..., None]
    return jnp.transpose(result, (1, 0, 2)).reshape(capacity, columns).astype(jnp.bfloat16)


VMEM = pl.BlockSpec(memory_space=pltpu.VMEM)
HBM = pl.BlockSpec(memory_space=pltpu.HBM)
TOP_BITS = 14.875


def gather(tokens, keep_list, counts):
    slots = keep_list.shape[0]
    token = lax.broadcasted_iota(jnp.int32, (tokens.shape[0], slots), 0)
    pick = lax.optimization_barrier((token == keep_list[None, :]).astype(jnp.bfloat16))
    rows = lax.dot_general(pick, tokens, (((0,), (0,)), ((), ())), preferred_element_type=jnp.float32)
    last = lax.broadcasted_iota(jnp.int32, rows.shape, 0) == slots - 1
    return jnp.where(last, counts[0].astype(jnp.float32), rows).astype(jnp.bfloat16)


def load_kernel(w_hbm, out_ref, sem):
    copy = pltpu.make_async_copy(w_hbm, out_ref, sem)
    copy.start()
    copy.wait()


def core_stride(shards, group):
    return shards // group if shards % group == 0 else 0


def toward(me, k, shards):
    return me ^ k if shards & (shards - 1) == 0 else (me + k) % shards


def step(j, core, shards):
    return shards - j if j and core % 2 else j


def own_kernel(shards, group, *refs):
    chunks, w_ref, (pick_ref, acc_ref) = refs[:shards], refs[shards], refs[shards + 1 :]
    slots, width = chunks[0].shape
    capacity = slots // 2
    kept = capacity * shards
    tp = lax.axis_index("tp")
    core = lax.rem(tp, group)
    line = lax.div(tp, group)
    stride = core_stride(shards, group)
    shard = [lax.rem(k + core * stride - line + shards, shards) for k in range(shards)]
    count = [chunks[k][slots - 1 : slots, :slots].astype(jnp.float32) for k in range(shards)]
    row = lax.broadcasted_iota(jnp.int32, (kept, slots), 0)
    rank = ((row % capacity) * shards + row // capacity).astype(jnp.float32)
    slot = lax.broadcasted_iota(jnp.int32, (kept, slots), 1).astype(jnp.float32)
    first = rank - slot
    picks = []
    for k in range(shards):
        start = jnp.zeros_like(count[k])
        for j in range(shards):
            if j != k:
                start += jnp.where(shard[j] < shard[k], count[j], 0.0)
        hit = (first == start) & (slot < count[k])
        picks.append(jnp.where(hit, 1.0, 0.0).astype(jnp.bfloat16))
        pick_ref[:, k * slots : (k + 1) * slots] = picks[k]
    rows = jnp.dot(
        jnp.concatenate(picks, axis=1),
        jnp.concatenate([chunk[...] for chunk in chunks], axis=0),
        preferred_element_type=jnp.float32,
    ).astype(jnp.bfloat16)
    where = pl.multiple_of(core * width, width)
    for kind in range(3):
        acc_ref[kind] = jnp.dot(
            rows, w_ref[kind, pl.ds(where, width), :], preferred_element_type=jnp.float32
        )


def rest_kernel(shards, group, heads, *refs):
    count = shards * (group - 1)
    halves = [refs[shards * p : shards * (p + 1)] for p in range(group - 1)]
    pick_ref, acc_ref, w_ref = refs[count : count + 3]
    outs = refs[count + 3 :]
    slots = pick_ref.shape[1] // shards
    width = w_ref.shape[1] // group
    kept = slots // 2 * shards
    blocks = shards // heads
    block_rows = kept // blocks
    stride = core_stride(shards, group)
    core = lax.rem(lax.axis_index("tp"), group)
    me = lax.axis_index("seq")
    rows = []
    for p in range(1, group):
        order = [(k + p * stride) % shards for k in range(shards)]
        pick = jnp.concatenate([pick_ref[:, o * slots : (o + 1) * slots] for o in order], axis=1)
        block = jnp.concatenate([half[...] for half in halves[p - 1]], axis=0)
        rows.append(jnp.dot(pick, block, preferred_element_type=jnp.float32).astype(jnp.bfloat16))
    total = 2 * kept + block_rows
    pad = outs[0].shape[0] - total
    dests = [me]
    for k in range(1, shards):
        dest = toward(me, step(k, 0, shards), shards)
        for c in range(1, group):
            dest = jnp.where(core == c, toward(me, step(k, c, shards), shards), dest)
        dests.append(dest)
    exponents = []
    for at, kind in enumerate((1, 2, 0)):
        acc = acc_ref[kind]
        for p in range(1, group):
            where = pl.multiple_of(lax.rem(core + p, group) * width, width)
            acc += jnp.dot(
                rows[p - 1], w_ref[kind, pl.ds(where, width), :], preferred_element_type=jnp.float32
            )
        most = jnp.maximum(jnp.max(jnp.abs(acc), axis=0, keepdims=True), 2.0**-112)
        exponent = jnp.floor(jnp.log2(most)) + 1.0
        exponents.append(exponent)
        value = jnp.round(acc * jnp.exp2(TOP_BITS - exponent)).astype(jnp.int32)
        for k, dest in enumerate(dests):
            mine = of_head(value, lax.rem(dest, heads), heads)
            if kind:
                outs[k][at * kept : (at + 1) * kept, :] = mine.astype(jnp.int16)
            else:
                block = lax.div(dest, heads)
                part = mine[:block_rows, :]
                for b in range(1, blocks):
                    part = jnp.where(block == b, mine[b * block_rows : (b + 1) * block_rows, :], part)
                outs[k][2 * kept : total, :] = part.astype(jnp.int16)

    index = lax.broadcasted_iota(jnp.int32, (pad, heads * HD), 0)
    tail = jnp.zeros((pad, heads * HD), jnp.float32)
    for at, exponent in enumerate(exponents):
        tail = jnp.where(index == at, exponent, tail)
    tail = tail.astype(jnp.int32)
    for k, dest in enumerate(dests):
        outs[k][total:, :] = of_head(tail, lax.rem(dest, heads), heads).astype(jnp.int16)


def of_head(value, head, heads):
    mine = value[:, :HD]
    for h in range(1, heads):
        mine = jnp.where(head == h, value[:, h * HD : (h + 1) * HD], mine)
    return mine


def attended(query, key, value, first_row, shards):
    capacity = key.shape[0] // shards
    scores = lax.dot_general(
        query, key, (((1,), (1,)), ((), ())), preferred_element_type=jnp.float32
    ) * (HD ** (-0.5))
    q_row = lax.broadcasted_iota(jnp.int32, scores.shape, 0) + first_row
    k_row = lax.broadcasted_iota(jnp.int32, scores.shape, 1)
    q_rank = lax.rem(q_row, capacity) * shards + lax.div(q_row, capacity)
    k_rank = lax.rem(k_row, capacity) * shards + lax.div(k_row, capacity)
    scores = jnp.where(k_rank > q_rank, -jnp.inf, scores)
    top = jnp.max(scores, axis=1, keepdims=True)
    expo = jnp.exp(scores - top)
    numer = jnp.dot(expo.astype(jnp.bfloat16), value, preferred_element_type=jnp.float32)
    return (numer / jnp.sum(expo, axis=1, keepdims=True)).astype(jnp.bfloat16)


def leaving_kernel(shards, heads, kept, *refs):
    parts, outs = refs[:shards], refs[shards : shards + heads - 1]
    key_ref, value_ref, query_ref = refs[shards + heads - 1 :]
    capacity = kept // shards
    me = lax.axis_index("seq")
    block_rows = kept // (shards // heads)
    total = 2 * kept + block_rows
    block = lax.div(me, heads)
    scales = [
        jnp.exp2(p[total:, :].astype(jnp.int32).astype(jnp.float32) - TOP_BITS) for p in parts
    ]

    def summed(i, lo, hi):
        acc = None
        for p, scale in zip(parts, scales):
            part = p[lo:hi, :].astype(jnp.int32).astype(jnp.float32) * scale[i : i + 1, :]
            acc = part if acc is None else acc + part
        return acc

    def rows_of(owner, rows):
        mine = rows[:capacity, :]
        for o in range(1, heads):
            mine = jnp.where(owner == o, rows[o * capacity : (o + 1) * capacity, :], mine)
        return mine.astype(jnp.bfloat16)

    query = summed(2, 2 * kept, total)
    key = summed(0, 0, kept).astype(jnp.bfloat16)
    value = summed(1, kept, 2 * kept).astype(jnp.bfloat16)
    key_ref[...] = key
    value_ref[...] = value
    head = lax.rem(me, heads)
    query_ref[...] = rows_of(head, query)
    for k in range(1, heads):
        owner = lax.rem(head + k, heads)
        first_row = block * block_rows + owner * capacity
        outs[k - 1][...] = attended(rows_of(owner, query), key, value, first_row, shards)


def staying_kernel(shards, key_ref, value_ref, query_ref, out_ref):
    first_row = lax.axis_index("seq") * query_ref.shape[0]
    out_ref[...] = attended(query_ref[...], key_ref[...], value_ref[...], first_row, shards)


def by_features(shards, tp, tokens, w_qkv, keep_list, counts):
    group = tp // shards
    slots = keep_list.shape[0]
    capacity = slots // 2
    kept = capacity * shards
    heads = w_qkv.shape[2] // HD
    axes = ("seq", "tp")
    params = pltpu.CompilerParams(vmem_limit_bytes=32 * 1024 * 1024)

    def device(s, line, core):
        return s * tp + line * group + core

    packed = gather(tokens, keep_list, counts)
    stride = core_stride(shards, group)
    every = [(s, line, c) for s in range(shards) for line in range(shards) for c in range(group)]
    own = []
    for k in range(shards):
        pairs = [
            (device(s, line, c), device(line, (k + c * stride - s) % shards, c))
            for s, line, c in every
        ]
        own.append(lax.ppermute(packed, axes, pairs))
    others = []
    for p in range(1, group):
        pairs = [
            (line * group + (c + p) % group, line * group + c)
            for line in range(shards)
            for c in range(group)
        ]
        for k in range(shards):
            others.append(lax.ppermute(own[k], "tp", pairs))
    weights = jnp.transpose(w_qkv, (1, 0, 2))
    weights = pl.pallas_call(
        load_kernel,
        out_shape=jax.ShapeDtypeStruct(weights.shape, weights.dtype),
        in_specs=[HBM],
        out_specs=VMEM,
        scratch_shapes=[pltpu.SemaphoreType.DMA],
        compiler_params=pltpu.CompilerParams(vmem_limit_bytes=51 * 1024 * 1024),
        name="load",
    )(weights)
    pick, acc = pl.pallas_call(
        functools.partial(own_kernel, shards, group),
        out_shape=[
            jax.ShapeDtypeStruct((kept, shards * slots), jnp.bfloat16),
            jax.ShapeDtypeStruct((3, kept, heads * HD), jnp.float32),
        ],
        in_specs=[VMEM] * (shards + 1),
        out_specs=[VMEM] * 2,
        compiler_params=params,
        name="own",
    )(*own, weights)
    blocks = shards // heads
    payload = 2 * kept + kept // blocks + 8
    partial = pl.pallas_call(
        functools.partial(rest_kernel, shards, group, heads),
        out_shape=[jax.ShapeDtypeStruct((payload, HD), jnp.int16)] * shards,
        in_specs=[VMEM] * (shards * (group - 1) + 3),
        out_specs=[VMEM] * shards,
        compiler_params=params,
        name="rest",
    )(*others, pick, acc, weights)
    parts = [partial[0]]
    for k in range(1, shards):
        pairs = [
            (device(s, line, c), device(toward(s, step(k, c, shards), shards), line, c))
            for s, line, c in every
        ]
        parts.append(lax.ppermute(partial[k], ("seq", "tp"), pairs))
    *leaving, key, value, query = pl.pallas_call(
        functools.partial(leaving_kernel, shards, heads, kept),
        out_shape=[
            jax.ShapeDtypeStruct((rows, HD), jnp.bfloat16)
            for rows in (capacity,) * (heads - 1) + (kept, kept, capacity)
        ],
        in_specs=[VMEM] * shards,
        out_specs=[VMEM] * (heads + 2),
        compiler_params=params,
        name="leaving",
    )(*parts)
    staying = pl.pallas_call(
        functools.partial(staying_kernel, shards),
        out_shape=jax.ShapeDtypeStruct((capacity, HD), jnp.bfloat16),
        in_specs=[VMEM] * 3,
        out_specs=VMEM,
        compiler_params=params,
        name="staying",
    )(key, value, query)
    arrived = [staying]
    for k in range(1, heads):
        pairs = [
            (b * heads + h, b * heads + (h + k) % heads) for b in range(blocks) for h in range(heads)
        ]
        arrived.append(lax.ppermute(leaving[k - 1], "seq", pairs))
    mine = lax.rem(lax.axis_index("seq"), heads)
    columns = []
    for h in range(heads):
        column = arrived[0]
        for k in range(1, heads):
            column = jnp.where(lax.rem(mine - k + heads, heads) == h, arrived[k], column)
        columns.append(column)
    return jnp.concatenate(columns, axis=1)


def fits(mesh):
    shards, tp = mesh.shape["seq"], mesh.shape["tp"]
    return tp % shards == 0 and tp > shards


def solution(mesh):
    shards, tp = mesh.shape["seq"], mesh.shape["tp"]

    def on_device(tokens, w_qkv, keep_list, counts):
        heads = w_qkv.shape[2] // HD
        if fits(mesh) and shards % heads == 0:
            return by_features(shards, tp, tokens, w_qkv, keep_list, counts)
        return by_rows(tokens, w_qkv, keep_list, counts)

    in_specs = (P("seq", "tp"), P("seq", None, "tp"), P("seq"), P("seq"))
    out_specs = P("seq", "tp")
    return jax.shard_map(
        on_device, mesh=mesh, in_specs=in_specs, out_specs=out_specs, check_vma=False
    )
```

```python
import functools

import jax
import jax.numpy as jnp
from jax import lax
from jax.experimental import pallas as pl
from jax.experimental.pallas import tpu as pltpu
from jax.sharding import PartitionSpec as P

HD = 128


def entering(value, axis, join, neutral):
    count, mine = (lax.axis_size(axis), lax.axis_index(axis))
    pieces = lax.all_gather(value, axis)
    so_far = jnp.full_like(value, 0) + jnp.asarray(neutral, value.dtype)

    def lap(position, so_far):
        longer = join(so_far, pieces[position])
        return jnp.where(position < mine, longer, so_far)

    return lax.fori_loop(0, count - 1, lap, so_far)


def add_sums(earlier, later):
    return earlier + later


def by_rows(tokens, w_qkv, keep_list, counts):
    shards = lax.axis_size("seq")
    my_index = lax.axis_index("seq")
    tok_dev = tokens.shape[0]
    slots = keep_list.shape[0]
    capacity = slots // 2
    per_peer = slots // shards
    head_dim = HD
    columns = w_qkv.shape[2]
    local_heads = columns // head_dim
    offset = entering(counts, "seq", add_sums, jnp.zeros_like(counts))[0]
    peers = jnp.arange(shards, dtype=jnp.int32)[:, None]
    rounds = jnp.arange(per_peer, dtype=jnp.int32)[None, :]
    local_slot = (peers - offset) % shards + rounds * shards
    live = local_slot < counts[0]
    token_index = keep_list[local_slot]
    ranks = jnp.where(live, offset + local_slot, -1).astype(jnp.int32)
    positions = my_index * tok_dev + token_index
    meta = jnp.stack([positions, ranks], axis=2)
    picked = jnp.where(live[:, :, None], tokens[token_index], jnp.zeros((), tokens.dtype))
    arrived, arrived_meta = (
        lax.all_to_all(picked, "seq", split_axis=0, concat_axis=0, tiled=True),
        lax.all_to_all(meta, "seq", split_axis=0, concat_axis=0, tiled=True),
    )
    arrived_meta = arrived_meta.reshape(shards * per_peer, 2)
    arrived_rank = arrived_meta[:, 1]
    target = jnp.where(arrived_rank >= 0, arrived_rank // shards, capacity)
    flat = arrived.reshape(shards * per_peer, arrived.shape[2])
    kept = jnp.zeros((capacity, flat.shape[1]), flat.dtype).at[target].set(flat, mode="drop")
    kept_pos = jnp.zeros((capacity,), jnp.int32).at[target].set(arrived_meta[:, 0], mode="drop")
    full_rows = lax.all_gather(kept, "tp", axis=1, tiled=True)
    piece = lax.all_gather(w_qkv, "seq", axis=0, tiled=True)
    part_rows = lax.slice_in_dim(full_rows, 0, piece.shape[0], axis=1)
    projected = jnp.einsum(
        "rd,dgc->rgc", part_rows, piece, preferred_element_type=jnp.float32
    ).astype(jnp.bfloat16)
    queries = projected[:, 0].reshape(capacity, local_heads, head_dim)
    key_values = projected[:, 1:]
    scale = head_dim ** (-0.5)
    all_kv, all_pos = (
        lax.all_gather(key_values, "seq", axis=0, tiled=True),
        lax.all_gather(kept_pos, "seq", axis=0, tiled=True),
    )
    total_keys = all_kv.shape[0]
    keys_all = all_kv[:, 0].reshape(total_keys, local_heads, head_dim)
    values_all = all_kv[:, 1].reshape(total_keys, local_heads, head_dim)
    scores = (
        jnp.einsum("qhd,khd->hqk", queries, keys_all, preferred_element_type=jnp.float32) * scale
    )
    masked = all_pos[None, None, :] > kept_pos[None, :, None]
    scores = jnp.where(masked, -jnp.inf, scores)
    top = jnp.max(scores, axis=2, keepdims=True)
    expo = jnp.exp(scores - top)
    numer = jnp.einsum(
        "hqk,khd->hqd", expo.astype(jnp.bfloat16), values_all, preferred_element_type=jnp.float32
    )
    result = numer / jnp.sum(expo, axis=2)[..., None]
    return jnp.transpose(result, (1, 0, 2)).reshape(capacity, columns).astype(jnp.bfloat16)


VMEM = pl.BlockSpec(memory_space=pltpu.VMEM)
HBM = pl.BlockSpec(memory_space=pltpu.HBM)
TOP_BITS = 14.875


def gather(tokens, keep_list, counts):
    slots = keep_list.shape[0]
    token = lax.broadcasted_iota(jnp.int32, (tokens.shape[0], slots), 0)
    pick = lax.optimization_barrier((token == keep_list[None, :]).astype(jnp.bfloat16))
    rows = lax.dot_general(pick, tokens, (((0,), (0,)), ((), ())), preferred_element_type=jnp.float32)
    last = lax.broadcasted_iota(jnp.int32, rows.shape, 0) == slots - 1
    return jnp.where(last, counts[0].astype(jnp.float32), rows).astype(jnp.bfloat16)


def load_kernel(w_hbm, out_ref, sem):
    copy = pltpu.make_async_copy(w_hbm, out_ref, sem)
    copy.start()
    copy.wait()


def core_stride(shards, group):
    return shards // group if shards % group == 0 else 0


def toward(me, k, shards):
    return (me + k) % shards


def step(j, core, shards):
    return shards - j if j and core % 2 else j


def own_kernel(shards, group, *refs):
    chunks, w_ref, (pick_ref, acc_ref) = refs[:shards], refs[shards], refs[shards + 1 :]
    slots, width = chunks[0].shape
    capacity = slots // 2
    kept = capacity * shards
    tp = lax.axis_index("tp")
    core = lax.rem(tp, group)
    line = lax.div(tp, group)
    stride = core_stride(shards, group)
    shard = [lax.rem(k + core * stride - line + shards, shards) for k in range(shards)]
    count = [chunks[k][slots - 1 : slots, :slots].astype(jnp.float32) for k in range(shards)]
    row = lax.broadcasted_iota(jnp.int32, (kept, slots), 0)
    rank = ((row % capacity) * shards + row // capacity).astype(jnp.float32)
    slot = lax.broadcasted_iota(jnp.int32, (kept, slots), 1).astype(jnp.float32)
    first = rank - slot
    picks = []
    for k in range(shards):
        start = jnp.zeros_like(count[k])
        for j in range(shards):
            if j != k:
                start += jnp.where(shard[j] < shard[k], count[j], 0.0)
        hit = (first == start) & (slot < count[k])
        picks.append(jnp.where(hit, 1.0, 0.0).astype(jnp.bfloat16))
        pick_ref[:, k * slots : (k + 1) * slots] = picks[k]
    rows = jnp.dot(
        jnp.concatenate(picks, axis=1),
        jnp.concatenate([chunk[...] for chunk in chunks], axis=0),
        preferred_element_type=jnp.float32,
    ).astype(jnp.bfloat16)
    where = pl.multiple_of(core * width, width)
    for kind in range(3):
        acc_ref[kind] = jnp.dot(
            rows, w_ref[kind, pl.ds(where, width), :], preferred_element_type=jnp.float32
        )


def rest_kernel(shards, group, heads, *refs):
    count = shards * (group - 1)
    halves = [refs[shards * p : shards * (p + 1)] for p in range(group - 1)]
    pick_ref, acc_ref, w_ref = refs[count : count + 3]
    outs = refs[count + 3 :]
    slots = pick_ref.shape[1] // shards
    width = w_ref.shape[1] // group
    kept = slots // 2 * shards
    blocks = shards // heads
    block_rows = kept // blocks
    stride = core_stride(shards, group)
    core = lax.rem(lax.axis_index("tp"), group)
    me = lax.axis_index("seq")
    rows = []
    for p in range(1, group):
        order = [(k + p * stride) % shards for k in range(shards)]
        pick = jnp.concatenate([pick_ref[:, o * slots : (o + 1) * slots] for o in order], axis=1)
        block = jnp.concatenate([half[...] for half in halves[p - 1]], axis=0)
        rows.append(jnp.dot(pick, block, preferred_element_type=jnp.float32).astype(jnp.bfloat16))
    total = 2 * kept + block_rows
    pad = outs[0].shape[0] - total
    dests = [me]
    for k in range(1, shards):
        dest = toward(me, step(k, 0, shards), shards)
        for c in range(1, group):
            dest = jnp.where(core == c, toward(me, step(k, c, shards), shards), dest)
        dests.append(dest)
    exponents = []
    for at, kind in enumerate((1, 2, 0)):
        acc = acc_ref[kind]
        for p in range(1, group):
            where = pl.multiple_of(lax.rem(core + p, group) * width, width)
            acc += jnp.dot(
                rows[p - 1], w_ref[kind, pl.ds(where, width), :], preferred_element_type=jnp.float32
            )
        most = jnp.maximum(jnp.max(jnp.abs(acc), axis=0, keepdims=True), 2.0**-112)
        exponent = jnp.floor(jnp.log2(most)) + 1.0
        exponents.append(exponent)
        value = jnp.round(acc * jnp.exp2(TOP_BITS - exponent)).astype(jnp.int32)
        for k, dest in enumerate(dests):
            mine = of_head(value, lax.rem(dest, heads), heads)
            if kind:
                outs[k][at * kept : (at + 1) * kept, :] = mine.astype(jnp.int16)
            else:
                block = lax.div(dest, heads)
                part = mine[:block_rows, :]
                for b in range(1, blocks):
                    part = jnp.where(block == b, mine[b * block_rows : (b + 1) * block_rows, :], part)
                outs[k][2 * kept : total, :] = part.astype(jnp.int16)

    index = lax.broadcasted_iota(jnp.int32, (pad, heads * HD), 0)
    tail = jnp.zeros((pad, heads * HD), jnp.float32)
    for at, exponent in enumerate(exponents):
        tail = jnp.where(index == at, exponent, tail)
    tail = tail.astype(jnp.int32)
    for k, dest in enumerate(dests):
        outs[k][total:, :] = of_head(tail, lax.rem(dest, heads), heads).astype(jnp.int16)


def of_head(value, head, heads):
    mine = value[:, :HD]
    for h in range(1, heads):
        mine = jnp.where(head == h, value[:, h * HD : (h + 1) * HD], mine)
    return mine


def attend_kernel(shards, heads, kept, *refs):
    parts, outs = refs[:shards], refs[shards:]
    capacity = kept // shards
    me = lax.axis_index("seq")
    block_rows = kept // (shards // heads)
    total = 2 * kept + block_rows
    block = lax.div(me, heads)
    scales = [
        jnp.exp2(p[total:, :].astype(jnp.int32).astype(jnp.float32) - TOP_BITS) for p in parts
    ]

    def summed(i, lo, hi):
        acc = None
        for p, scale in zip(parts, scales):
            part = p[lo:hi, :].astype(jnp.int32).astype(jnp.float32) * scale[i : i + 1, :]
            acc = part if acc is None else acc + part
        return acc.astype(jnp.bfloat16)

    key, value, query = summed(0, 0, kept), summed(1, kept, 2 * kept), summed(2, 2 * kept, total)
    scores = lax.dot_general(
        query, key, (((1,), (1,)), ((), ())), preferred_element_type=jnp.float32
    ) * (HD ** (-0.5))
    q_row = lax.broadcasted_iota(jnp.int32, scores.shape, 0) + block * block_rows
    k_row = lax.broadcasted_iota(jnp.int32, scores.shape, 1)
    q_rank = lax.rem(q_row, capacity) * shards + lax.div(q_row, capacity)
    k_rank = lax.rem(k_row, capacity) * shards + lax.div(k_row, capacity)
    scores = jnp.where(k_rank > q_rank, -jnp.inf, scores)
    top = jnp.max(scores, axis=1, keepdims=True)
    expo = jnp.exp(scores - top)
    numer = jnp.dot(expo.astype(jnp.bfloat16), value, preferred_element_type=jnp.float32)
    result = numer / jnp.sum(expo, axis=1, keepdims=True)
    head = lax.rem(me, heads)
    for k in range(heads):
        owner = lax.rem(head + k, heads)
        piece = result[:capacity, :]
        for o in range(1, heads):
            piece = jnp.where(owner == o, result[o * capacity : (o + 1) * capacity, :], piece)
        outs[k][...] = piece.astype(jnp.bfloat16)


def by_features(shards, tp, tokens, w_qkv, keep_list, counts):
    group = tp // shards
    slots = keep_list.shape[0]
    capacity = slots // 2
    kept = capacity * shards
    heads = w_qkv.shape[2] // HD
    axes = ("seq", "tp")
    params = pltpu.CompilerParams(vmem_limit_bytes=32 * 1024 * 1024)

    def device(s, line, core):
        return s * tp + line * group + core

    packed = gather(tokens, keep_list, counts)
    stride = core_stride(shards, group)
    every = [(s, line, c) for s in range(shards) for line in range(shards) for c in range(group)]
    own = []
    for k in range(shards):
        pairs = [
            (device(s, line, c), device(line, (k + c * stride - s) % shards, c))
            for s, line, c in every
        ]
        own.append(lax.ppermute(packed, axes, pairs))
    others = []
    for p in range(1, group):
        pairs = [
            (line * group + (c + p) % group, line * group + c)
            for line in range(shards)
            for c in range(group)
        ]
        for k in range(shards):
            others.append(lax.ppermute(own[k], "tp", pairs))
    weights = jnp.transpose(w_qkv, (1, 0, 2))
    weights = pl.pallas_call(
        load_kernel,
        out_shape=jax.ShapeDtypeStruct(weights.shape, weights.dtype),
        in_specs=[HBM],
        out_specs=VMEM,
        scratch_shapes=[pltpu.SemaphoreType.DMA],
        compiler_params=pltpu.CompilerParams(vmem_limit_bytes=51 * 1024 * 1024),
        name="load",
    )(weights)
    pick, acc = pl.pallas_call(
        functools.partial(own_kernel, shards, group),
        out_shape=[
            jax.ShapeDtypeStruct((kept, shards * slots), jnp.bfloat16),
            jax.ShapeDtypeStruct((3, kept, heads * HD), jnp.float32),
        ],
        in_specs=[VMEM] * (shards + 1),
        out_specs=[VMEM] * 2,
        compiler_params=params,
        name="own",
    )(*own, weights)
    blocks = shards // heads
    payload = 2 * kept + kept // blocks + 8
    partial = pl.pallas_call(
        functools.partial(rest_kernel, shards, group, heads),
        out_shape=[jax.ShapeDtypeStruct((payload, HD), jnp.int16)] * shards,
        in_specs=[VMEM] * (shards * (group - 1) + 3),
        out_specs=[VMEM] * shards,
        compiler_params=params,
        name="rest",
    )(*others, pick, acc, weights)
    parts = [partial[0]]
    for k in range(1, shards):
        pairs = [
            (device(s, line, c), device(toward(s, step(k, c, shards), shards), line, c))
            for s, line, c in every
        ]
        parts.append(lax.ppermute(partial[k], ("seq", "tp"), pairs))
    pieces = pl.pallas_call(
        functools.partial(attend_kernel, shards, heads, kept),
        out_shape=[jax.ShapeDtypeStruct((capacity, HD), jnp.bfloat16)] * heads,
        in_specs=[VMEM] * shards,
        out_specs=[VMEM] * heads,
        compiler_params=params,
        name="attend",
    )(*parts)
    arrived = [pieces[0]]
    for k in range(1, heads):
        pairs = [
            (b * heads + h, b * heads + (h + k) % heads) for b in range(blocks) for h in range(heads)
        ]
        arrived.append(lax.ppermute(pieces[k], "seq", pairs))
    mine = lax.rem(lax.axis_index("seq"), heads)
    columns = []
    for h in range(heads):
        column = arrived[0]
        for k in range(1, heads):
            column = jnp.where(lax.rem(mine - k + heads, heads) == h, arrived[k], column)
        columns.append(column)
    return jnp.concatenate(columns, axis=1)


def fits(mesh):
    shards, tp = mesh.shape["seq"], mesh.shape["tp"]
    return tp % shards == 0 and tp > shards


def solution(mesh):
    shards, tp = mesh.shape["seq"], mesh.shape["tp"]

    def on_device(tokens, w_qkv, keep_list, counts):
        heads = w_qkv.shape[2] // HD
        if fits(mesh) and shards % heads == 0:
            return by_features(shards, tp, tokens, w_qkv, keep_list, counts)
        return by_rows(tokens, w_qkv, keep_list, counts)

    in_specs = (P("seq", "tp"), P("seq", None, "tp"), P("seq"), P("seq"))
    out_specs = P("seq", "tp")
    return jax.shard_map(
        on_device, mesh=mesh, in_specs=in_specs, out_specs=out_specs, check_vma=False
    )
```
